512 devices in a mesh: grp: 2 (over y), row: 16 (over x, core), col: 16 (over z).
Axes of the slice: x: 8, y: 2, z: 16, core: 2. Of those that a mesh axis runs over, the one named last changes fastest.
The devices are a block of a 8x8x16 slice.
Arguments:
- eigvec: float32 [65536, 4096], P(('grp', 'row'), 'col'), parts along dimension 0, may hold values from -6 to 6
- reflectors: float32 [8, 65536], P(None, ('grp', 'row', 'col')), parts along dimension 1, may hold values from -6 to 6
- offsets: int32 [16], P('grp'), parts along dimension 0, may hold values from 1 to 255
Outputs:
- transformed: float32 [65536, 4096], P(('grp', 'row'), 'col'), parts along dimension 0
The draws below stay inside these ranges and needn't reach their ends.
There are 2 independent parts, one for each index of `grp`. The reference program is written for one: setup_inputs(seed, part) draws one part's arguments, and reference() takes and returns one part's arrays. A program takes and returns all parts, laid end to end along the dimension named above; each array names one. Nothing has to cross between parts.
All inputs are finite; a program needn't handle non-finite values.
Results may differ from the reference program's by a relative error of at most 0.00013.
Values sent between devices are 32-bit elements; how exact they have to be, the bound alone decides.
A program may use at most 64 MiB of HBM per device.

```python
import jax
import jax.numpy as jnp
from jax import lax

B = 256
NEV = 4096
SWEEPS = 8
NR = 32768


def place_ends(drawn, rng, least, largest):
    index_at = [jax.random.randint(jax.random.fold_in(rng, axis), (), 0, length) for axis, length in enumerate(drawn.shape)]
    main_axis = drawn.shape.index(max(drawn.shape))
    neighbour = index_at[:main_axis] + [(index_at[main_axis] + 1) % drawn.shape[main_axis]] + index_at[main_axis + 1:]
    return drawn.at[tuple(index_at)].set(least).at[tuple(neighbour)].set(largest)


def steps_of(rng, extent, split, low, high):
    level = 1.0
    for position, blocks in split:
        heights = jax.random.uniform(jax.random.fold_in(jax.random.fold_in(rng, 6), position), (blocks,), jnp.float32, low / len(split), high / len(split))
        level = level * jnp.repeat(jnp.exp(heights), extent[position] // blocks).reshape((-1,) + (1,) * (len(extent) - 1 - position))
    return level


def normal_values(own_key, shape, width, limit, shards=(), held_as=jnp.bfloat16):
    values = jax.random.normal(own_key, shape, jnp.float32) * width
    if len(shards) > 0:
        values = steps_of(own_key, shape, shards, -0.22, 0.18) * values
    return jnp.clip(values, min=-limit, max=limit).astype(held_as)


def setup_inputs(seed: int = 0, part: int = 0) -> dict:
    splits = jax.random.split(jax.random.key(seed), 4)
    own_keys = jax.random.split(jax.random.fold_in(splits[3], part), 4)
    return {
        "eigvec": normal_values(own_keys[0], (NR, NEV), 1.0, 6.0, ((0, 16), (1, 16)), jnp.float32),
        "reflectors": normal_values(own_keys[1], (SWEEPS, NR), 1.0, 6.0, ((1, 256),), jnp.float32),
        "offsets": place_ends(jax.random.randint(own_keys[2], (SWEEPS,), 1, B), jax.random.fold_in(own_keys[2], 1), 1, B - 1).astype(jnp.int32),
    }


def apply_update(row_block, householder, products, square_sums, usable):
    scaling = jnp.where(usable, 2.0 / jnp.where(usable, square_sums, 1.0), 0.0)
    return row_block - (scaling[:, None] * householder)[:, :, None] * products[:, None, :]


def reflect_update(row_block, householder, usable):
    square_sums = jnp.sum(householder * householder, axis=1)
    products = jnp.einsum("jb,jbc->jc", householder, row_block, precision=lax.Precision.HIGHEST)
    return apply_update(row_block, householder, products, square_sums, usable)


def reference(eigvec, reflectors, offsets):
    total_rows, columns = eigvec.shape
    blocks = total_rows // B - 1
    current = eigvec
    for sweep_index in range(SWEEPS):
        offset = offsets[sweep_index]
        row_block = lax.dynamic_slice_in_dim(current, offset, blocks * B, 0).reshape(blocks, B, columns)
        householder = lax.dynamic_slice_in_dim(reflectors[sweep_index], offset, blocks * B, 0).reshape(blocks, B)
        householder = householder.at[:, 0].set(1.0)
        usable = jnp.ones((blocks,), jnp.bool_)
        updated = reflect_update(row_block, householder, usable)
        current = lax.dynamic_update_slice_in_dim(current, updated.reshape(blocks * B, columns), offset, 0)
    return current
```

```python
import functools

import jax
import jax.numpy as jnp
from jax import lax
from jax.experimental import pallas as pl
from jax.experimental.pallas import tpu as pltpu
from jax.sharding import PartitionSpec as P

B = 256
MESH = pl.DeviceIdType.MESH
HIGHEST = lax.Precision.HIGHEST


def masked_sets(tile, off, first_row, group):
    row = first_row + lax.broadcasted_iota(jnp.int32, tile.shape, 1) - group * B
    tile = jnp.where(row == off, 1.0, tile)
    before = row < off
    return jnp.concatenate([jnp.where(before, tile, 0.0), jnp.where(before, 0.0, tile)], 0)


def offset_column(off_ref, sweeps):
    which = lax.broadcasted_iota(jnp.int32, (sweeps, 1), 0)
    off = jnp.zeros((sweeps, 1), jnp.int32)
    for s in range(sweeps):
        off = jnp.where(which == s, off_ref[s], off)
    return off


def coupling_kernel(
    n_col, n_row, off_ref, refl_ref, eig_ref, sets_ref, coef_ref,
    sets, own, above, below, chain, plus_send, minus_send, recv, row_send, row_recv,
):
    sweeps, chunk = refl_ref.shape
    rows, cols = eig_ref.shape
    blocks, parts = rows // B, cols // 128
    per_block = B // chunk
    col = lax.axis_index("col")
    row = lax.axis_index("row")
    right, left = lax.rem(col + 1, n_col), lax.rem(col + n_col - 1, n_col)
    has_above, has_below = row > 0, row < n_row - 1

    barrier = pltpu.get_barrier_semaphore()
    for peer in (right, left):
        pl.semaphore_signal(barrier, inc=1, device_id={"col": peer}, device_id_type=MESH)

    @pl.when(has_above)
    def _():
        pl.semaphore_signal(barrier, inc=1, device_id={"row": row - 1}, device_id_type=MESH)

    @pl.when(has_below)
    def _():
        pl.semaphore_signal(barrier, inc=1, device_id={"row": row + 1}, device_id_type=MESH)

    pl.semaphore_wait(barrier, 2 + jnp.where(has_above, 1, 0) + jnp.where(has_below, 1, 0))

    plus, minus = n_col // 2, n_col - 1 - n_col // 2

    def send(source, index, sem, peer):
        copy = pltpu.make_async_remote_copy(
            src_ref=source, dst_ref=sets.at[index], send_sem=sem, recv_sem=recv.at[index],
            device_id={"col": peer}, device_id_type=MESH,
        )
        copy.start()
        return copy

    def arrived(index):
        pltpu.make_async_remote_copy(
            src_ref=sets.at[index], dst_ref=sets.at[index], send_sem=plus_send.at[0], recv_sem=recv.at[index],
            device_id={"col": right}, device_id_type=MESH,
        ).wait_recv()

    copies = [send(refl_ref, col, plus_send.at[0], left), send(refl_ref, col, minus_send.at[0], right)]
    sets[col] = refl_ref[...]
    for t in range(1, plus + 1):
        index = lax.rem(col + t, n_col)
        arrived(index)
        if t < plus:
            copies.append(send(sets.at[index], index, plus_send.at[t], left))
    for t in range(1, minus + 1):
        index = lax.rem(col + n_col - t, n_col)
        arrived(index)
        if t < minus:
            copies.append(send(sets.at[index], index, minus_send.at[t], right))

    off = offset_column(off_ref, sweeps)
    wide = 2 * sweeps
    zeros = jnp.zeros((sweeps, B), jnp.float32)
    own[...] = jnp.zeros_like(own)
    for b in range(blocks):
        tile = jnp.concatenate([sets[b * per_block + i] for i in range(per_block)], 1)
        v = masked_sets(tile, off, b * B, b)
        x = eig_ref[b * B : (b + 1) * B]
        p = jnp.dot(v, x, precision=HIGHEST, preferred_element_type=jnp.float32)
        for h in range(parts):
            own[h, b * sweeps : (b + 2) * sweeps] += p[:, h * 128 : (h + 1) * 128]
        nt = (((1,), (1,)), ((), ()))
        lower = jnp.concatenate([zeros, v, jnp.zeros((128 - 3 * sweeps, B), jnp.float32)], 0)
        upper = jnp.concatenate([v, jnp.zeros((128 - 2 * sweeps, B), jnp.float32)], 0)
        own[parts, b * sweeps : (b + 1) * sweeps] += lax.dot_general(
            v[:sweeps], lower, nt, precision=HIGHEST, preferred_element_type=jnp.float32
        )
        own[parts, (b + 1) * sweeps : (b + 2) * sweeps] += lax.dot_general(
            v[sweeps:], upper, nt, precision=HIGHEST, preferred_element_type=jnp.float32
        )

    def to_row(buffer, i, peer):
        return pltpu.make_async_remote_copy(
            src_ref=own, dst_ref=buffer, send_sem=row_send.at[i], recv_sem=row_recv.at[i],
            device_id={"row": peer}, device_id_type=MESH,
        )

    down = to_row(above, 0, jnp.minimum(row + 1, n_row - 1))
    up = to_row(below, 1, jnp.maximum(row - 1, 0))

    @pl.when(has_below)
    def _():
        down.start()

    @pl.when(has_above)
    def _():
        up.start()

    groups = blocks + 1
    own_at = groups - 2
    total = chain.shape[1] // sweeps
    chain[...] = jnp.zeros_like(chain)
    chain[:, own_at * sweeps : (own_at + groups) * sweeps] = own[...]

    @pl.when(has_above)
    def _():
        down.wait_recv()
        chain[:, : (own_at + 1) * sweeps] += above[:, sweeps:]

    @pl.when(has_below)
    def _():
        up.wait_recv()
        chain[:, (own_at + groups - 1) * sweeps : (own_at + 2 * groups - 2) * sweeps] += below[:, : (groups - 1) * sweeps]

    place = lax.broadcasted_iota(jnp.int32, (total, 1), 0)
    first = jnp.where(has_above, 0, own_at + 1)
    last = jnp.where(has_below, own_at + 2 * groups - 2, own_at + groups - 1)
    valid = (place >= first) & (place < last)
    most = coef_ref.shape[1] // sweeps
    solved = []
    for s in range(sweeps):
        gram = chain[parts, pl.ds(s, total, stride=sweeps), :]
        acc = jnp.concatenate([chain[h, pl.ds(s, total, stride=sweeps), :] for h in range(parts)], 1)
        for p in range(s):
            before, here, after = solved[p]
            acc -= gram[:, sweeps + p : sweeps + p + 1] * here
            acc -= gram[:, p : p + 1] * before
            acc -= gram[:, 2 * sweeps + p : 2 * sweeps + p + 1] * after
        square = gram[:, sweeps + s : sweeps + s + 1]
        tau = jnp.where(valid, 2.0 / jnp.where(valid, square, 1.0), 0.0)
        here = tau * acc
        solved.append((pltpu.roll(here, 1, 0), here, pltpu.roll(here, total - 1, 0)))
        kept = pltpu.roll(here, total - own_at, 0)[:most]
        for h in range(parts):
            coef_ref[h, pl.ds(s, most, stride=sweeps), :] = kept[:, h * 128 : (h + 1) * 128]
    for i in range(n_col):
        sets_ref[i] = sets[i]

    for copy in copies:
        copy.wait_send()

    @pl.when(has_below)
    def _():
        down.wait_send()

    @pl.when(has_above)
    def _():
        up.wait_send()


def update_kernel(off_ref, sets_ref, coef_ref, eig_ref, out_ref):
    per_block, sweeps, _ = sets_ref.shape
    b = pl.program_id(0)
    off = offset_column(off_ref, sweeps)
    tile = jnp.concatenate([sets_ref[i] for i in range(per_block)], 1)
    v = masked_sets(tile, off, b * B, b)
    z = jnp.concatenate([coef_ref[h, pl.ds(pl.multiple_of(b * sweeps, sweeps), 2 * sweeps), :] for h in range(coef_ref.shape[0])], 1)
    out_ref[...] = eig_ref[...] - lax.dot_general(
        v, z, (((0,), (0,)), ((), ())), precision=HIGHEST, preferred_element_type=jnp.float32
    )


def body(n_col, n_row, eigvec, reflectors, offsets):
    rows, cols = eigvec.shape
    sweeps, chunk = reflectors.shape
    groups = rows // B + 1
    total, most = (-(-count // 8) * 8 for count in (3 * groups - 3, groups))
    vmem, smem = pl.BlockSpec(memory_space=pltpu.VMEM), pl.BlockSpec(memory_space=pltpu.SMEM)
    parts = cols // 128
    message = (parts + 1, groups * sweeps, 128)
    dma, f32 = pltpu.SemaphoreType.DMA, jnp.float32
    sets, coef = pl.pallas_call(
        functools.partial(coupling_kernel, n_col, n_row),
        out_shape=(jax.ShapeDtypeStruct((n_col, sweeps, chunk), f32), jax.ShapeDtypeStruct((parts, most * sweeps, 128), f32)),
        in_specs=[smem, vmem, vmem],
        out_specs=(vmem, vmem),
        scratch_shapes=[
            pltpu.VMEM((n_col, sweeps, chunk), f32),
            pltpu.VMEM(message, f32),
            pltpu.VMEM(message, f32),
            pltpu.VMEM(message, f32),
            pltpu.VMEM((parts + 1, total * sweeps, 128), f32),
            dma((n_col,)),
            dma((n_col,)),
            dma((n_col,)),
            dma((2,)),
            dma((2,)),
        ],
        compiler_params=pltpu.CompilerParams(collective_id=0, has_side_effects=True),
        name="coupling",
    )(offsets, reflectors, eigvec)
    per_block = B // chunk
    return pl.pallas_call(
        update_kernel,
        out_shape=jax.ShapeDtypeStruct(eigvec.shape, f32),
        grid=(rows // B,),
        in_specs=[
            smem,
            pl.BlockSpec((per_block, sweeps, chunk), lambda b: (b, 0, 0)),
            pl.BlockSpec((parts, most * sweeps, 128), lambda b: (0, 0, 0)),
            pl.BlockSpec((B, cols), lambda b: (b, 0)),
        ],
        out_specs=pl.BlockSpec((B, cols), lambda b: (b, 0)),
        name="update",
    )(offsets, sets, coef, eigvec)


def solution(mesh):
    in_specs = (P(("grp", "row"), "col"), P(None, ("grp", "row", "col")), P("grp"))
    out_specs = P(("grp", "row"), "col")
    step = functools.partial(body, mesh.shape["col"], mesh.shape["row"])
    return jax.shard_map(step, mesh=mesh, in_specs=in_specs, out_specs=out_specs, check_vma=False)
```

```python
import functools

import jax
import jax.numpy as jnp
from jax import lax
from jax.experimental import pallas as pl
from jax.experimental.pallas import tpu as pltpu
from jax.sharding import PartitionSpec as P

B = 256
MESH = pl.DeviceIdType.MESH
HIGHEST = lax.Precision.HIGHEST


def masked_sets(tile, off, first_row, group):
    row = first_row + lax.broadcasted_iota(jnp.int32, tile.shape, 1) - group * B
    tile = jnp.where(row == off, 1.0, tile)
    before = row < off
    return jnp.concatenate([jnp.where(before, tile, 0.0), jnp.where(before, 0.0, tile)], 0)


def offset_column(off_ref, sweeps):
    which = lax.broadcasted_iota(jnp.int32, (sweeps, 1), 0)
    off = jnp.zeros((sweeps, 1), jnp.int32)
    for s in range(sweeps):
        off = jnp.where(which == s, off_ref[s], off)
    return off


def coupling_kernel(
    n_col, n_row, off_ref, refl_ref, eig_ref, sets_ref, coef_ref,
    sets, own, above, below, chain, sent, recv, row_send, row_recv, zero,
):
    sweeps, chunk = refl_ref.shape
    rows, cols = eig_ref.shape
    blocks, parts = rows // B, cols // 128
    per_block = B // chunk
    col = lax.axis_index("col")
    row = lax.axis_index("row")
    has_above, has_below = row > 0, row < n_row - 1
    end = n_col - 1

    barrier = pltpu.get_barrier_semaphore()

    def greet(axis, peer):
        pl.semaphore_signal(barrier, inc=1, device_id={axis: peer}, device_id_type=MESH)

    @pl.when(has_above)
    def _():
        greet("row", row - 1)

    @pl.when(has_below)
    def _():
        greet("row", row + 1)

    @pl.when(col == 0)
    def _():
        greet("col", 1)
        greet("col", end)

    @pl.when(col == 1)
    def _():
        greet("col", 2)

    peers = jnp.where(has_above, 1, 0) + jnp.where(has_below, 1, 0) + jnp.where(col == 0, 0, 1) + jnp.where(col == end, 1, 0)
    pl.semaphore_wait(barrier, peers)

    def block_to(peer):
        return pltpu.make_async_remote_copy(
            src_ref=refl_ref, dst_ref=sets.at[col], send_sem=sent.at[peer], recv_sem=recv.at[col],
            device_id={"col": peer}, device_id_type=MESH,
        )

    def arrived(index):
        pltpu.make_async_remote_copy(
            src_ref=refl_ref, dst_ref=sets.at[index], send_sem=sent.at[index], recv_sem=recv.at[index],
            device_id={"col": index}, device_id_type=MESH,
        ).wait_recv()

    @pl.when((col == 1) | (col == end))
    def _():
        block_to(0).start()

    @pl.when((col >= 2) & (col < end))
    def _():
        greet("col", col + 1)

    for peer in range(1, end):

        @pl.when(peer < col)
        def _():
            block_to(peer).start()

    @pl.when((col >= 2) & (col < end))
    def _():
        pl.semaphore_wait(zero, 1)
        block_to(0).start()

    sets[col] = refl_ref[...]
    off = offset_column(off_ref, sweeps)
    own[...] = jnp.zeros_like(own)
    nt = (((1,), (1,)), ((), ()))
    zeros = jnp.zeros((sweeps, B), jnp.float32)

    def project(b):
        tile = jnp.concatenate([sets[b * per_block + i] for i in range(per_block)], 1)
        v = masked_sets(tile, off, b * B, b)
        x = eig_ref[b * B : (b + 1) * B]
        p = jnp.dot(v, x, precision=HIGHEST, preferred_element_type=jnp.float32)
        for h in range(parts):
            own[h, b * sweeps : (b + 2) * sweeps] += p[:, h * 128 : (h + 1) * 128]
        lower = jnp.concatenate([zeros, v, jnp.zeros((128 - 3 * sweeps, B), jnp.float32)], 0)
        upper = jnp.concatenate([v, jnp.zeros((128 - 2 * sweeps, B), jnp.float32)], 0)
        own[parts, b * sweeps : (b + 1) * sweeps] += lax.dot_general(
            v[:sweeps], lower, nt, precision=HIGHEST, preferred_element_type=jnp.float32
        )
        own[parts, (b + 1) * sweeps : (b + 2) * sweeps] += lax.dot_general(
            v[sweeps:], upper, nt, precision=HIGHEST, preferred_element_type=jnp.float32
        )

    for peer in range(n_col):

        @pl.when(peer > col)
        def _():
            arrived(peer)
            block_to(peer).start()

        if 2 <= peer < end:

            @pl.when(peer == col + 1)
            def _():
                pl.semaphore_signal(zero, inc=1, device_id={"col": peer}, device_id_type=MESH)

        if peer % per_block == per_block - 1:

            @pl.when(peer - per_block + 1 >= col)
            def _():
                project(peer // per_block)

    for b in range(blocks):
        for peer in range(b * per_block, (b + 1) * per_block):

            @pl.when(peer < col)
            def _():
                arrived(peer)

        @pl.when(b * per_block < col)
        def _():
            project(b)

    def to_row(buffer, i, peer):
        return pltpu.make_async_remote_copy(
            src_ref=own, dst_ref=buffer, send_sem=row_send.at[i], recv_sem=row_recv.at[i],
            device_id={"row": peer}, device_id_type=MESH,
        )

    down = to_row(above, 0, jnp.minimum(row + 1, n_row - 1))
    up = to_row(below, 1, jnp.maximum(row - 1, 0))

    @pl.when(has_below)
    def _():
        down.start()

    @pl.when(has_above)
    def _():
        up.start()

    groups = blocks + 1
    own_at = groups - 2
    total = chain.shape[1] // sweeps
    chain[...] = jnp.zeros_like(chain)
    chain[:, own_at * sweeps : (own_at + groups) * sweeps] = own[...]

    @pl.when(has_above)
    def _():
        down.wait_recv()
        chain[:, : (own_at + 1) * sweeps] += above[:, sweeps:]

    @pl.when(has_below)
    def _():
        up.wait_recv()
        chain[:, (own_at + groups - 1) * sweeps : (own_at + 2 * groups - 2) * sweeps] += below[:, : (groups - 1) * sweeps]

    place = lax.broadcasted_iota(jnp.int32, (total, 1), 0)
    first = jnp.where(has_above, 0, own_at + 1)
    last = jnp.where(has_below, own_at + 2 * groups - 2, own_at + groups - 1)
    valid = (place >= first) & (place < last)
    most = coef_ref.shape[1] // sweeps
    solved = []
    for s in range(sweeps):
        gram = chain[parts, pl.ds(s, total, stride=sweeps), :]
        acc = jnp.concatenate([chain[h, pl.ds(s, total, stride=sweeps), :] for h in range(parts)], 1)
        for p in range(s):
            before, here, after = solved[p]
            acc -= gram[:, sweeps + p : sweeps + p + 1] * here
            acc -= gram[:, p : p + 1] * before
            acc -= gram[:, 2 * sweeps + p : 2 * sweeps + p + 1] * after
        square = gram[:, sweeps + s : sweeps + s + 1]
        tau = jnp.where(valid, 2.0 / jnp.where(valid, square, 1.0), 0.0)
        here = tau * acc
        solved.append((pltpu.roll(here, 1, 0), here, pltpu.roll(here, total - 1, 0)))
        kept = pltpu.roll(here, total - own_at, 0)[:most]
        for h in range(parts):
            coef_ref[h, pl.ds(s, most, stride=sweeps), :] = kept[:, h * 128 : (h + 1) * 128]
    for i in range(n_col):
        sets_ref[i] = sets[i]

    for peer in range(n_col):

        @pl.when(peer != col)
        def _():
            block_to(peer).wait_send()

    @pl.when(has_below)
    def _():
        down.wait_send()

    @pl.when(has_above)
    def _():
        up.wait_send()


def halves(x):
    high = x.astype(jnp.bfloat16)
    return high, (x - high.astype(jnp.float32)).astype(jnp.bfloat16)


def update_kernel(off_ref, sets_ref, coef_ref, eig_ref, out_ref):
    count, sweeps, chunk = sets_ref.shape
    per_block = B // chunk
    off = offset_column(off_ref, sweeps)
    blocks = count // per_block
    for i in range(blocks):
        b = pl.program_id(0) * blocks + i
        tile = jnp.concatenate([sets_ref[i * per_block + j] for j in range(per_block)], 1)
        v_high, v_low = halves(masked_sets(tile, off, b * B, b))
        rows = pl.ds(pl.multiple_of(b * sweeps, sweeps), 2 * sweeps)
        z_high, z_low = halves(jnp.concatenate([coef_ref[h, rows, :] for h in range(coef_ref.shape[0])], 1))
        at = pl.ds(i * B, B)
        out_ref[at] = eig_ref[at] - lax.dot_general(
            jnp.concatenate([v_high, v_low, v_high], 0),
            jnp.concatenate([z_high, z_high, z_low], 0),
            (((0,), (0,)), ((), ())),
            preferred_element_type=jnp.float32,
        )


def body(n_col, n_row, eigvec, reflectors, offsets):
    rows, cols = eigvec.shape
    sweeps, chunk = reflectors.shape
    groups = rows // B + 1
    total, most = (-(-count // 8) * 8 for count in (3 * groups - 3, groups))
    vmem, smem = pl.BlockSpec(memory_space=pltpu.VMEM), pl.BlockSpec(memory_space=pltpu.SMEM)
    parts = cols // 128
    message = (parts + 1, groups * sweeps, 128)
    dma, f32 = pltpu.SemaphoreType.DMA, jnp.float32
    sets, coef = pl.pallas_call(
        functools.partial(coupling_kernel, n_col, n_row),
        out_shape=(jax.ShapeDtypeStruct((n_col, sweeps, chunk), f32), jax.ShapeDtypeStruct((parts, most * sweeps, 128), f32)),
        in_specs=[smem, vmem, vmem],
        out_specs=(vmem, vmem),
        scratch_shapes=[
            pltpu.VMEM((n_col, sweeps, chunk), f32),
            pltpu.VMEM(message, f32),
            pltpu.VMEM(message, f32),
            pltpu.VMEM(message, f32),
            pltpu.VMEM((parts + 1, total * sweeps, 128), f32),
            dma((n_col,)),
            dma((n_col,)),
            dma((2,)),
            dma((2,)),
            pltpu.SemaphoreType.REGULAR,
        ],
        compiler_params=pltpu.CompilerParams(collective_id=0, has_side_effects=True),
        name="coupling",
    )(offsets, reflectors, eigvec)
    steps = 2
    return pl.pallas_call(
        update_kernel,
        out_shape=jax.ShapeDtypeStruct(eigvec.shape, f32),
        grid=(steps,),
        in_specs=[
            smem,
            pl.BlockSpec((n_col // steps, sweeps, chunk), lambda b: (b, 0, 0)),
            pl.BlockSpec((parts, most * sweeps, 128), lambda b: (0, 0, 0)),
            pl.BlockSpec((rows // steps, cols), lambda b: (b, 0)),
        ],
        out_specs=pl.BlockSpec((rows // steps, cols), lambda b: (b, 0)),
        name="update",
    )(offsets, sets, coef, eigvec)


def solution(mesh):
    in_specs = (P(("grp", "row"), "col"), P(None, ("grp", "row", "col")), P("grp"))
    out_specs = P(("grp", "row"), "col")
    step = functools.partial(body, mesh.shape["col"], mesh.shape["row"])
    return jax.shard_map(step, mesh=mesh, in_specs=in_specs, out_specs=out_specs, check_vma=False)
```

```python
import functools

import jax
import jax.numpy as jnp
from jax import lax
from jax.experimental import pallas as pl
from jax.experimental.pallas import tpu as pltpu
from jax.sharding import PartitionSpec as P

B = 256
MESH = pl.DeviceIdType.MESH
HIGHEST = lax.Precision.HIGHEST


def masked_sets(tile, off, first_row, group):
    row = first_row + lax.broadcasted_iota(jnp.int32, tile.shape, 1) - group * B
    tile = jnp.where(row == off, 1.0, tile)
    before = row < off
    return jnp.concatenate([jnp.where(before, tile, 0.0), jnp.where(before, 0.0, tile)], 0)


def offset_column(off_ref, sweeps):
    which = lax.broadcasted_iota(jnp.int32, (sweeps, 1), 0)
    off = jnp.zeros((sweeps, 1), jnp.int32)
    for s in range(sweeps):
        off = jnp.where(which == s, off_ref[s], off)
    return off


def coupling_kernel(
    n_col, n_row, off_ref, refl_ref, eig_ref, sets_ref, coef_ref, x_ref,
    sets, own, chain, sent, passed, recv, row_send, row_recv, loaded,
):
    sweeps, chunk = refl_ref.shape
    rows, cols = eig_ref.shape
    blocks, parts = rows // B, cols // 128
    per_block = B // chunk
    col = lax.axis_index("col")
    row = lax.axis_index("row")
    has_above, has_below = row > 0, row < n_row - 1
    end = n_col - 1

    load = pltpu.make_async_copy(eig_ref, x_ref, loaded)
    load.start()
    barrier = pltpu.get_barrier_semaphore()

    def greet(axis, peer):
        pl.semaphore_signal(barrier, inc=1, device_id={axis: peer}, device_id_type=MESH)

    @pl.when(has_above)
    def _():
        greet("row", row - 1)

    @pl.when(has_below)
    def _():
        greet("row", row + 1)

    @pl.when(col == 0)
    def _():
        greet("col", 1)
        greet("col", end)

    @pl.when(col == 1)
    def _():
        greet("col", 2)

    peers = jnp.where(has_above, 1, 0) + jnp.where(has_below, 1, 0) + jnp.where(col == 0, 0, 1) + jnp.where(col == end, 1, 0)
    pl.semaphore_wait(barrier, peers)

    def block_to(peer):
        return pltpu.make_async_remote_copy(
            src_ref=refl_ref, dst_ref=sets.at[col], send_sem=sent.at[peer], recv_sem=recv.at[col],
            device_id={"col": peer}, device_id_type=MESH,
        )

    def passed_on(index):
        return pltpu.make_async_remote_copy(
            src_ref=sets.at[index], dst_ref=sets.at[index], send_sem=passed.at[index], recv_sem=recv.at[index],
            device_id={"col": 0}, device_id_type=MESH,
        )

    def arrived(index):
        pltpu.make_async_remote_copy(
            src_ref=refl_ref, dst_ref=sets.at[index], send_sem=sent.at[index], recv_sem=recv.at[index],
            device_id={"col": index}, device_id_type=MESH,
        ).wait_recv()

    @pl.when((col == 1) | (col == end))
    def _():
        block_to(0).start()

    @pl.when((col >= 2) & (col < end))
    def _():
        greet("col", col + 1)

    for peer in range(1, end):

        @pl.when(peer < col)
        def _():
            block_to(peer).start()

    sets[col] = refl_ref[...]
    off = offset_column(off_ref, sweeps)
    own[...] = jnp.zeros_like(own)
    nt = (((1,), (1,)), ((), ()))
    zeros = jnp.zeros((sweeps, B), jnp.float32)

    def project(b):
        tile = jnp.concatenate([sets[b * per_block + i] for i in range(per_block)], 1)
        v = masked_sets(tile, off, b * B, b)
        x = x_ref[b * B : (b + 1) * B]
        p = jnp.dot(v, x, precision=HIGHEST, preferred_element_type=jnp.float32)
        for h in range(parts):
            own[h, b * sweeps : (b + 2) * sweeps] += p[:, h * 128 : (h + 1) * 128]
        lower = jnp.concatenate([zeros, v, jnp.zeros((128 - 3 * sweeps, B), jnp.float32)], 0)
        upper = jnp.concatenate([v, jnp.zeros((128 - 2 * sweeps, B), jnp.float32)], 0)
        own[parts, b * sweeps : (b + 1) * sweeps] += lax.dot_general(
            v[:sweeps], lower, nt, precision=HIGHEST, preferred_element_type=jnp.float32
        )
        own[parts, (b + 1) * sweeps : (b + 2) * sweeps] += lax.dot_general(
            v[sweeps:], upper, nt, precision=HIGHEST, preferred_element_type=jnp.float32
        )

    groups = blocks + 1
    seam, other = (groups - 2) * sweeps, (2 * groups - 3) * sweeps
    early = (groups - 2) * sweeps

    def down(part):
        first, after = ((sweeps, early), (early, groups * sweeps))[part]
        return pltpu.make_async_remote_copy(
            src_ref=own.at[:, first:after], dst_ref=chain.at[:, first - sweeps : after - sweeps],
            send_sem=row_send.at[part], recv_sem=row_recv.at[part],
            device_id={"row": jnp.minimum(row + 1, n_row - 1)}, device_id_type=MESH,
        )

    def up(part):
        first, after = ((0, early), (early, (groups - 1) * sweeps))[part]
        return pltpu.make_async_remote_copy(
            src_ref=own.at[:, first:after], dst_ref=chain.at[:, other + first : other + after],
            send_sem=row_send.at[2 + part], recv_sem=row_recv.at[2 + part],
            device_id={"row": jnp.maximum(row - 1, 0)}, device_id_type=MESH,
        )

    def to_rows(part):
        @pl.when(has_below)
        def _():
            down(part).start()

        @pl.when(has_above)
        def _():
            up(part).start()

    load.wait()
    for peer in range(n_col):

        @pl.when(peer > col)
        def _():
            arrived(peer)
            block_to(peer).start()

        if 2 <= peer < end:

            @pl.when(col == 1)
            def _():
                passed_on(peer).start()

        if peer % per_block == per_block - 1:

            @pl.when(peer - per_block + 1 >= col)
            def _():
                project(peer // per_block)

            if peer // per_block == blocks - 2:

                @pl.when(col == 0)
                def _():
                    to_rows(0)

    for b in range(blocks):
        for peer in range(b * per_block, (b + 1) * per_block):

            @pl.when(peer < col)
            def _():
                arrived(peer)

        @pl.when(b * per_block < col)
        def _():
            project(b)

        if b == blocks - 2:

            @pl.when(col > 0)
            def _():
                to_rows(0)

    to_rows(1)
    chain[:, seam + sweeps : other] = own[:, sweeps : (groups - 1) * sweeps]
    tail = other + (groups - 1) * sweeps
    chain[:, tail:] = jnp.zeros((parts + 1, chain.shape[1] - tail, 128), jnp.float32)

    @pl.when(jnp.logical_not(has_above))
    def _():
        chain[:, : seam + sweeps] = jnp.zeros((parts + 1, seam + sweeps, 128), jnp.float32)

    @pl.when(jnp.logical_not(has_below))
    def _():
        chain[:, other:tail] = jnp.zeros((parts + 1, tail - other, 128), jnp.float32)

    @pl.when(has_above)
    def _():
        down(0).wait_recv()
        down(1).wait_recv()

    @pl.when(has_below)
    def _():
        up(0).wait_recv()
        up(1).wait_recv()

    chain[:, seam : seam + sweeps] += own[:, :sweeps]
    chain[:, other : other + sweeps] += own[:, (groups - 1) * sweeps :]

    own_at = groups - 2
    total = chain.shape[1] // sweeps
    place = lax.broadcasted_iota(jnp.int32, (total, 1), 0)
    first = jnp.where(has_above, 0, own_at + 1)
    last = jnp.where(has_below, own_at + 2 * groups - 2, own_at + groups - 1)
    valid = (place >= first) & (place < last)
    most = coef_ref.shape[1] // sweeps
    solved = []
    for s in range(sweeps):
        gram = chain[parts, pl.ds(s, total, stride=sweeps), :]
        acc = jnp.concatenate([chain[h, pl.ds(s, total, stride=sweeps), :] for h in range(parts)], 1)
        for p in range(s):
            before, here, after = solved[p]
            acc -= gram[:, sweeps + p : sweeps + p + 1] * here
            acc -= gram[:, p : p + 1] * before
            acc -= gram[:, 2 * sweeps + p : 2 * sweeps + p + 1] * after
        square = gram[:, sweeps + s : sweeps + s + 1]
        tau = jnp.where(valid, 2.0 / jnp.where(valid, square, 1.0), 0.0)
        here = tau * acc
        solved.append((pltpu.roll(here, 1, 0), here, pltpu.roll(here, total - 1, 0)))
        kept = pltpu.roll(here, total - own_at, 0)[:most]
        for h in range(parts):
            coef_ref[h, pl.ds(s, most, stride=sweeps), :] = kept[:, h * 128 : (h + 1) * 128]
    for i in range(n_col):
        sets_ref[i] = sets[i]

    for peer in range(n_col):

        @pl.when((peer != col) & ((peer > 0) | (col == 1) | (col == end)))
        def _():
            block_to(peer).wait_send()

        if 2 <= peer < end:

            @pl.when(col == 1)
            def _():
                passed_on(peer).wait_send()

    for part in range(2):

        @pl.when(has_below)
        def _():
            down(part).wait_send()

        @pl.when(has_above)
        def _():
            up(part).wait_send()


def halves(x):
    high = x.astype(jnp.bfloat16)
    return high, (x - high.astype(jnp.float32)).astype(jnp.bfloat16)


def update_kernel(off_ref, sets_ref, coef_ref, eig_ref, out_ref):
    count, sweeps, chunk = sets_ref.shape
    per_block = B // chunk
    off = offset_column(off_ref, sweeps)
    blocks = count // per_block
    for i in range(blocks):
        b = pl.program_id(0) * blocks + i
        tile = jnp.concatenate([sets_ref[i * per_block + j] for j in range(per_block)], 1)
        v_high, v_low = halves(masked_sets(tile, off, b * B, b))
        rows = pl.ds(pl.multiple_of(b * sweeps, sweeps), 2 * sweeps)
        z_high, z_low = halves(jnp.concatenate([coef_ref[h, rows, :] for h in range(coef_ref.shape[0])], 1))
        out_ref[pl.ds(i * B, B)] = eig_ref[pl.ds(pl.multiple_of(b * B, B), B)] - lax.dot_general(
            jnp.concatenate([v_high, v_low, v_high], 0),
            jnp.concatenate([z_high, z_high, z_low], 0),
            (((0,), (0,)), ((), ())),
            preferred_element_type=jnp.float32,
        )


def body(n_col, n_row, eigvec, reflectors, offsets):
    rows, cols = eigvec.shape
    sweeps, chunk = reflectors.shape
    groups = rows // B + 1
    total, most = (-(-count // 8) * 8 for count in (3 * groups - 3, groups))
    vmem, smem = pl.BlockSpec(memory_space=pltpu.VMEM), pl.BlockSpec(memory_space=pltpu.SMEM)
    parts = cols // 128
    message = (parts + 1, groups * sweeps, 128)
    dma, f32 = pltpu.SemaphoreType.DMA, jnp.float32
    held = pl.pallas_call(
        functools.partial(coupling_kernel, n_col, n_row),
        out_shape=(
            pltpu.VMEM((n_col, sweeps, chunk), f32),
            pltpu.VMEM((parts, most * sweeps, 128), f32),
            pltpu.VMEM(eigvec.shape, f32),
        ),
        in_specs=[smem, vmem, pl.BlockSpec(memory_space=pl.ANY)],
        out_specs=(vmem, vmem, vmem),
        scratch_shapes=[
            pltpu.VMEM((n_col, sweeps, chunk), f32),
            pltpu.VMEM(message, f32),
            pltpu.VMEM((parts + 1, total * sweeps, 128), f32),
            dma((n_col,)),
            dma((n_col,)),
            dma((n_col,)),
            dma((4,)),
            dma((4,)),
            dma,
        ],
        compiler_params=pltpu.CompilerParams(collective_id=0, has_side_effects=True),
        name="coupling",
    )(offsets, reflectors, eigvec)
    steps = 2
    return pl.pallas_call(
        update_kernel,
        out_shape=jax.ShapeDtypeStruct(eigvec.shape, f32),
        grid=(steps,),
        in_specs=[
            smem,
            pl.BlockSpec((n_col // steps, sweeps, chunk), lambda b: (b, 0, 0)),
            pl.BlockSpec((parts, most * sweeps, 128), lambda b: (0, 0, 0)),
            vmem,
        ],
        out_specs=pl.BlockSpec((rows // steps, cols), lambda b: (b, 0)),
        name="update",
    )(offsets, *(pltpu.with_memory_space_constraint(array, pltpu.VMEM) for array in held))


def solution(mesh):
    in_specs = (P(("grp", "row"), "col"), P(None, ("grp", "row", "col")), P("grp"))
    out_specs = P(("grp", "row"), "col")
    step = functools.partial(body, mesh.shape["col"], mesh.shape["row"])
    return jax.shard_map(step, mesh=mesh, in_specs=in_specs, out_specs=out_specs, check_vma=False)
```

```python
import functools

import jax
import jax.numpy as jnp
from jax import lax
from jax.experimental import pallas as pl
from jax.experimental.pallas import tpu as pltpu
from jax.sharding import PartitionSpec as P

B = 256
MESH = pl.DeviceIdType.MESH
HIGHEST = lax.Precision.HIGHEST


def masked_sets(tile, off, first_row, group):
    row = first_row + lax.broadcasted_iota(jnp.int32, tile.shape, 1) - group * B
    tile = jnp.where(row == off, 1.0, tile)
    before = row < off
    return jnp.concatenate([jnp.where(before, tile, 0.0), jnp.where(before, 0.0, tile)], 0)


def offset_column(off_ref, sweeps):
    which = lax.broadcasted_iota(jnp.int32, (sweeps, 1), 0)
    off = jnp.zeros((sweeps, 1), jnp.int32)
    for s in range(sweeps):
        off = jnp.where(which == s, off_ref[s], off)
    return off


def halves(x):
    high = x.astype(jnp.bfloat16)
    return high, (x - high.astype(jnp.float32)).astype(jnp.bfloat16)


def product(v, x):
    count = v.shape[0]
    v_high, v_low = halves(v)
    x_high, x_low = halves(x)
    both = jnp.dot(jnp.concatenate([v_high, v_low], 0), x_high, preferred_element_type=jnp.float32)
    return both[:count] + both[count:] + jnp.dot(v_high, x_low, preferred_element_type=jnp.float32)


def coupling_kernel(
    n_col, n_row, off_hbm, refl_hbm, eig_hbm, sets_ref, coef_ref, off_ref, x_ref,
    sets, own, chain, side, tails, off_smem, sent, passed, recv, row_send, row_recv, side_send, side_recv, tail_send, tail_recv, loaded,
):
    sweeps, chunk = refl_hbm.shape
    rows, cols = eig_hbm.shape
    blocks, parts = rows // B, cols // 128
    per_block = B // chunk
    col = lax.axis_index("col")
    row = lax.axis_index("row")
    has_above, has_below = row > 0, row < n_row - 1
    end = n_col - 1

    loads = [
        pltpu.make_async_copy(refl_hbm, sets.at[col], loaded.at[0]),
        pltpu.make_async_copy(off_hbm, off_smem, loaded.at[1]),
        pltpu.make_async_copy(eig_hbm, x_ref, loaded.at[2]),
    ]
    for load in loads:
        load.start()

    barrier = pltpu.get_barrier_semaphore()

    def greet(axis, peer):
        pl.semaphore_signal(barrier, inc=1, device_id={axis: peer}, device_id_type=MESH)

    @pl.when(has_above)
    def _():
        greet("row", row - 1)

    @pl.when(has_below)
    def _():
        greet("row", row + 1)

    @pl.when(col == 1)
    def _():
        greet("col", 2)

    peers = jnp.where(has_above, 1, 0) + jnp.where(has_below, 1, 0) + jnp.where(col == 0, 0, 1) + jnp.where(col == end, 1, 0)
    pl.semaphore_wait(barrier, peers)

    @pl.when(col == 0)
    def _():
        greet("col", 1)
        greet("col", end)

    @pl.when((col >= 2) & (col < end))
    def _():
        greet("col", col + 1)

    def remote(source, target, send_sem, recv_sem, **device):
        return pltpu.make_async_remote_copy(
            src_ref=source, dst_ref=target, send_sem=send_sem, recv_sem=recv_sem, device_id=device, device_id_type=MESH
        )

    def block_to(peer):
        return remote(sets.at[col], sets.at[col], sent.at[peer], recv.at[col], col=peer)

    def passed_on(index):
        return remote(sets.at[index], sets.at[index], passed.at[index], recv.at[index], col=0)

    def arrived(index):
        remote(sets.at[index], sets.at[index], sent.at[index], recv.at[index], col=index).wait_recv()

    above, below = jnp.maximum(row - 1, 0), jnp.minimum(row + 1, n_row - 1)

    def aside(place, peer_col, upward):
        slot, peer = (1, above) if upward else (0, below)
        return remote(sets.at[end], side.at[slot], side_send.at[place], side_recv.at[slot], row=peer, col=peer_col)

    def asides(place, peer_col, act):
        @pl.when(has_below)
        def _():
            act(aside(place, peer_col, False))

        @pl.when(has_above)
        def _():
            act(aside(place + 1, peer_col, True))

    def start(copy):
        copy.start()

    def sent_off(copy):
        copy.wait_send()

    loads[0].wait()

    @pl.when((col == 1) | (col == end))
    def _():
        block_to(0).start()

    @pl.when(col == end)
    def _():
        asides(2, 0, start)

    for peer in range(1, end):

        @pl.when(peer < col)
        def _():
            block_to(peer).start()

    @pl.when(col == end)
    def _():
        asides(0, col, start)

    loads[1].wait()
    off = offset_column(off_smem, sweeps)
    off_ref[...] = jnp.broadcast_to(off, off_ref.shape)
    own[...] = jnp.zeros_like(own)
    chain_rows = chain.shape[1]

    def project(tile, first, b, x):
        v = masked_sets(tile, off, first, b)
        p = product(v, x)
        padded = [jnp.zeros((sweeps, v.shape[1]), jnp.float32), v, jnp.zeros((128 - 3 * sweeps, v.shape[1]), jnp.float32)]
        g = lax.dot_general(
            v, jnp.concatenate(padded, 0), (((1,), (1,)), ((), ())), precision=HIGHEST, preferred_element_type=jnp.float32
        )
        g = jnp.concatenate([g[:sweeps], pltpu.roll(g[sweeps:], 128 - sweeps, 1)], 0)
        return [p[:, h * 128 : (h + 1) * 128] for h in range(parts)] + [g]

    def project_own(first_chunk, count):
        b = first_chunk // per_block
        tile = jnp.concatenate([sets[first_chunk + i] for i in range(count)], 1)
        terms = project(tile, first_chunk * chunk, b, x_ref[first_chunk * chunk : (first_chunk + count) * chunk])
        for h, term in enumerate(terms):
            own[h, b * sweeps : (b + 2) * sweeps] += term

    groups = blocks + 1
    seam, other = (groups - 2) * sweeps, (2 * groups - 3) * sweeps
    below_end = other + (groups - 1) * sweeps

    def down():
        return remote(own.at[:, sweeps:], chain.at[:, : seam + sweeps], row_send.at[0], row_recv.at[0], row=below)

    def up():
        source = own.at[:, : (groups - 1) * sweeps]
        return remote(source, chain.at[:, other:below_end], row_send.at[1], row_recv.at[1], row=above)

    def tail_down():
        return remote(x_ref.at[rows - chunk :], tails.at[0], tail_send.at[0], tail_recv.at[0], row=below)

    def tail_up():
        return remote(x_ref.at[rows - chunk :], tails.at[1], tail_send.at[1], tail_recv.at[1], row=above)

    def to_rows():
        @pl.when(has_below)
        def _():
            down().start()

        @pl.when(has_above)
        def _():
            up().start()

    loads[2].wait()

    @pl.when(has_below)
    def _():
        tail_down().start()

    @pl.when(has_above)
    def _():
        tail_up().start()

    halved = end - end % per_block
    for peer in range(n_col):

        @pl.when(peer > col)
        def _():
            arrived(peer)
            block_to(peer).start()

        if 2 <= peer < end:

            @pl.when(col == 1)
            def _():
                passed_on(peer).start()

        if peer % per_block == per_block - 1 and peer < end:

            @pl.when(peer - per_block + 1 >= col)
            def _():
                project_own(peer - per_block + 1, per_block)

        if halved <= peer < end:

            @pl.when(peer >= col)
            def _():
                project_own(peer, 1)

        if peer == end - 1:

            @pl.when(col == 0)
            def _():
                to_rows()

    @pl.when((col > 0) & (col < end))
    def _():
        asides(0, col, start)

    for first in [*range(0, halved, per_block), *range(halved, end)]:
        count = per_block if first < halved else 1
        for peer in range(first, first + count):

            @pl.when(peer < col)
            def _():
                arrived(peer)

        @pl.when(first < col)
        def _():
            project_own(first, count)

    @pl.when(col > 0)
    def _():
        to_rows()

    chain[:, seam + sweeps : other] = own[:, sweeps : (groups - 1) * sweeps]
    chain[:, below_end:] = jnp.zeros((parts + 1, chain_rows - below_end, 128), jnp.float32)

    @pl.when(jnp.logical_not(has_above))
    def _():
        chain[:, : seam + sweeps] = jnp.zeros((parts + 1, seam + sweeps, 128), jnp.float32)
        side[0] = jnp.zeros_like(side[0])
        tails[0] = jnp.zeros_like(tails[0])

    @pl.when(jnp.logical_not(has_below))
    def _():
        chain[:, other:below_end] = jnp.zeros((parts + 1, below_end - other, 128), jnp.float32)
        side[1] = jnp.zeros_like(side[1])
        tails[1] = jnp.zeros_like(tails[1])

    @pl.when(has_above)
    def _():
        tail_down().wait_recv()
        down().wait_recv()
        aside(0, col, False).wait_recv()

    @pl.when(has_below)
    def _():
        tail_up().wait_recv()
        up().wait_recv()
        aside(1, col, True).wait_recv()

    last = rows - chunk
    mine = project(sets[end], last, blocks - 1, x_ref[last:])
    theirs = [project(side[i], last, blocks - 1, tails[i]) for i in range(2)]
    for h in range(parts + 1):
        chain[h, seam : seam + sweeps] += own[h, :sweeps] + theirs[0][h][sweeps:]
        chain[h, seam - sweeps : seam] += theirs[0][h][:sweeps]
        chain[h, other - sweeps : other] += mine[h][:sweeps]
        chain[h, other : other + sweeps] += own[h, (groups - 1) * sweeps :] + mine[h][sweeps:]
        chain[h, below_end - sweeps : below_end] += theirs[1][h][:sweeps]

    own_at = groups - 2
    total = chain_rows // sweeps
    place = lax.broadcasted_iota(jnp.int32, (total, 1), 0)
    first = jnp.where(has_above, 0, own_at + 1)
    stop = jnp.where(has_below, own_at + 2 * groups - 2, own_at + groups - 1)
    valid = (place >= first) & (place < stop)
    most = coef_ref.shape[1] // sweeps
    solved = []
    for s in range(sweeps):
        gram = chain[parts, pl.ds(s, total, stride=sweeps), :]
        acc = jnp.concatenate([chain[h, pl.ds(s, total, stride=sweeps), :] for h in range(parts)], 1)
        for p in range(s):
            before, here, after = solved[p]
            acc -= gram[:, sweeps + p : sweeps + p + 1] * here
            acc -= gram[:, p : p + 1] * before
            acc -= gram[:, 2 * sweeps + p : 2 * sweeps + p + 1] * after
        square = gram[:, sweeps + s : sweeps + s + 1]
        tau = jnp.where(valid, 2.0 / jnp.where(valid, square, 1.0), 0.0)
        here = tau * acc
        solved.append((pltpu.roll(here, 1, 0), here, pltpu.roll(here, total - 1, 0)))
        kept = pltpu.roll(here, total - own_at, 0)[:most]
        for h in range(parts):
            coef_ref[h, pl.ds(s, most, stride=sweeps), :] = kept[:, h * 128 : (h + 1) * 128]
    for i in range(n_col):
        sets_ref[i] = sets[i]

    for peer in range(n_col):

        @pl.when((peer != col) & ((peer > 0) | (col == 1) | (col == end)))
        def _():
            block_to(peer).wait_send()

        if 2 <= peer < end:

            @pl.when(col == 1)
            def _():
                passed_on(peer).wait_send()

    @pl.when(col > 0)
    def _():
        asides(0, col, sent_off)

    @pl.when(col == end)
    def _():
        asides(2, 0, sent_off)

    @pl.when(has_below)
    def _():
        tail_down().wait_send()
        down().wait_send()

    @pl.when(has_above)
    def _():
        tail_up().wait_send()
        up().wait_send()


def update_kernel(off_ref, sets_ref, coef_ref, x_ref, out_hbm, out, out_sem):
    count, sweeps, chunk = sets_ref.shape
    per_block = B // chunk
    off = off_ref[:, :1]
    steps = out.shape[0]
    blocks = count // per_block // steps

    def write(step):
        return pltpu.make_async_copy(out.at[step], out_hbm.at[pl.ds(step * blocks * B, blocks * B)], out_sem.at[step])

    for step in range(steps):
        for i in range(blocks):
            b = step * blocks + i
            tile = jnp.concatenate([sets_ref[b * per_block + j] for j in range(per_block)], 1)
            v_high, v_low = halves(masked_sets(tile, off, b * B, b))
            z = [coef_ref[h, b * sweeps : (b + 2) * sweeps, :] for h in range(coef_ref.shape[0])]
            z_high, z_low = halves(jnp.concatenate(z, 1))
            out[step, i * B : (i + 1) * B] = x_ref[b * B : (b + 1) * B] - lax.dot_general(
                jnp.concatenate([v_high, v_low, v_high], 0),
                jnp.concatenate([z_high, z_high, z_low], 0),
                (((0,), (0,)), ((), ())),
                preferred_element_type=jnp.float32,
            )
        write(step).start()
    for step in range(steps):
        write(step).wait()


def body(n_col, n_row, eigvec, reflectors, offsets):
    rows, cols = eigvec.shape
    sweeps, chunk = reflectors.shape
    groups = rows // B + 1
    total, most = (-(-count // 8) * 8 for count in (3 * groups - 3, groups))
    vmem, hbm = pl.BlockSpec(memory_space=pltpu.VMEM), pl.BlockSpec(memory_space=pl.ANY)
    parts = cols // 128
    dma, f32 = pltpu.SemaphoreType.DMA, jnp.float32
    held = pl.pallas_call(
        functools.partial(coupling_kernel, n_col, n_row),
        out_shape=(
            pltpu.VMEM((n_col, sweeps, chunk), f32),
            pltpu.VMEM((parts, most * sweeps, 128), f32),
            pltpu.VMEM((sweeps, 128), jnp.int32),
            pltpu.VMEM(eigvec.shape, f32),
        ),
        in_specs=[hbm, hbm, hbm],
        out_specs=(vmem, vmem, vmem, vmem),
        scratch_shapes=[
            pltpu.VMEM((n_col, sweeps, chunk), f32),
            pltpu.VMEM((parts + 1, groups * sweeps, 128), f32),
            pltpu.VMEM((parts + 1, total * sweeps, 128), f32),
            pltpu.VMEM((2, sweeps, chunk), f32),
            pltpu.VMEM((2, chunk, cols), f32),
            pltpu.SMEM(offsets.shape, jnp.int32),
            dma((n_col,)),
            dma((n_col,)),
            dma((n_col,)),
            dma((2,)),
            dma((2,)),
            dma((4,)),
            dma((2,)),
            dma((2,)),
            dma((2,)),
            dma((3,)),
        ],
        compiler_params=pltpu.CompilerParams(collective_id=0, has_side_effects=True),
        name="coupling",
    )(offsets, reflectors, eigvec)
    sets, coef, off, x = (pltpu.with_memory_space_constraint(array, pltpu.VMEM) for array in held)
    steps = 4
    return pl.pallas_call(
        update_kernel,
        out_shape=jax.ShapeDtypeStruct(eigvec.shape, f32),
        in_specs=[vmem, vmem, vmem, vmem],
        out_specs=hbm,
        scratch_shapes=[pltpu.VMEM((steps, rows // steps, cols), f32), dma((steps,))],
        name="update",
    )(off, sets, coef, x)


def solution(mesh):
    in_specs = (P(("grp", "row"), "col"), P(None, ("grp", "row", "col")), P("grp"))
    out_specs = P(("grp", "row"), "col")
    step = functools.partial(body, mesh.shape["col"], mesh.shape["row"])
    return jax.shard_map(step, mesh=mesh, in_specs=in_specs, out_specs=out_specs, check_vma=False)
```

```python
import functools

import jax
import jax.numpy as jnp
from jax import lax
from jax.experimental import pallas as pl
from jax.experimental.pallas import tpu as pltpu
from jax.sharding import PartitionSpec as P

B = 256
MESH = pl.DeviceIdType.MESH
HIGHEST = lax.Precision.HIGHEST


def masked_sets(tile, off, first_row, group):
    row = first_row + lax.broadcasted_iota(jnp.int32, tile.shape, 1) - group * B
    tile = jnp.where(row == off, 1.0, tile)
    before = row < off
    return jnp.concatenate([jnp.where(before, tile, 0.0), jnp.where(before, 0.0, tile)], 0)


def offset_column(off_ref, sweeps):
    which = lax.broadcasted_iota(jnp.int32, (sweeps, 1), 0)
    off = jnp.zeros((sweeps, 1), jnp.int32)
    for s in range(sweeps):
        off = jnp.where(which == s, off_ref[s], off)
    return off


def halves(x):
    high = x.astype(jnp.bfloat16)
    return high, (x - high.astype(jnp.float32)).astype(jnp.bfloat16)


def product(v, x):
    count = v.shape[0]
    v_high, v_low = halves(v)
    x_high, x_low = halves(x)
    both = jnp.dot(jnp.concatenate([v_high, v_low], 0), x_high, preferred_element_type=jnp.float32)
    return both[:count] + both[count:] + jnp.dot(v_high, x_low, preferred_element_type=jnp.float32)


def coupling_kernel(
    n_col, n_row, off_hbm, refl_hbm, eig_hbm, sets_ref, coef_ref, off_ref, x_ref,
    sets, own, chain, side, tails, off_smem, sent, passed, recv, row_send, row_recv, side_send, side_recv, tail_send, tail_recv, loaded,
):
    sweeps, chunk = refl_hbm.shape
    rows, cols = eig_hbm.shape
    blocks, parts = rows // B, cols // 128
    per_block = B // chunk
    col = lax.axis_index("col")
    row = lax.axis_index("row")
    has_above, has_below = row > 0, row < n_row - 1
    end, head = n_col - 1, n_col - per_block
    apart = (row == 0) & (lax.axis_index("grp") == 0)

    loads = [
        pltpu.make_async_copy(refl_hbm, sets.at[col], loaded.at[0]),
        pltpu.make_async_copy(off_hbm, off_smem, loaded.at[1]),
        pltpu.make_async_copy(eig_hbm, x_ref, loaded.at[2]),
    ]
    for load in loads:
        load.start()

    barrier = pltpu.get_barrier_semaphore()

    def greet(axis, peer):
        pl.semaphore_signal(barrier, inc=1, device_id={axis: peer}, device_id_type=MESH)

    @pl.when(has_above)
    def _():
        greet("row", row - 1)

    @pl.when(has_below)
    def _():
        greet("row", row + 1)

    @pl.when(col == 0)
    def _():
        greet("col", 1)

    @pl.when((col == 1) & apart)
    def _():
        greet("col", 2)

    peers = jnp.where(has_above, 1, 0) + jnp.where(has_below, 1, 0) + jnp.where(col == 0, 0, 1) + jnp.where(col == end, 1, 0)
    pl.semaphore_wait(barrier, peers)

    @pl.when(col == 0)
    def _():
        greet("col", end)

    @pl.when(((col >= 2) | ((col == 1) & jnp.logical_not(apart))) & (col < end))
    def _():
        greet("col", col + 1)

    def remote(source, target, send_sem, recv_sem, **device):
        return pltpu.make_async_remote_copy(
            src_ref=source, dst_ref=target, send_sem=send_sem, recv_sem=recv_sem, device_id=device, device_id_type=MESH
        )

    def block_to(peer):
        return remote(sets.at[col], sets.at[col], sent.at[peer], recv.at[col], col=peer)

    def passed_on(index):
        return remote(sets.at[index], sets.at[index], passed.at[index], recv.at[index], col=0)

    def arrived(index):
        remote(sets.at[index], sets.at[index], sent.at[index], recv.at[index], col=index).wait_recv()

    above, below = jnp.maximum(row - 1, 0), jnp.minimum(row + 1, n_row - 1)

    def aside(which, peer_col, upward, extra=0):
        slot, peer = (1, above) if upward else (0, below)
        target, index = side.at[slot, which], slot * per_block + which
        return remote(sets.at[head + which], target, side_send.at[index + extra], side_recv.at[index], row=peer, col=peer_col)

    def asides(which, peer_col, act, extra=0):
        @pl.when(has_below)
        def _():
            act(aside(which, peer_col, False, extra))

        @pl.when(has_above)
        def _():
            act(aside(which, peer_col, True, extra))

    def start(copy):
        copy.start()

    def sent_off(copy):
        copy.wait_send()

    loads[0].wait()

    to_first = (col == 1) | (col == end) | ((col > 0) & jnp.logical_not(apart))

    @pl.when(to_first)
    def _():
        block_to(0).start()

    @pl.when(col == end)
    def _():
        asides(per_block - 1, 0, start, 2 * per_block)

    for peer in range(1, end):

        @pl.when(peer < col)
        def _():
            block_to(peer).start()

    for which in range(per_block):

        @pl.when(col == head + which)
        def _():
            asides(which, col, start)

    loads[1].wait()
    off = offset_column(off_smem, sweeps)
    off_ref[...] = jnp.broadcast_to(off, off_ref.shape)
    own[...] = jnp.zeros_like(own)
    chain_rows = chain.shape[1]

    def project(tile, first, b, x):
        v = masked_sets(tile, off, first, b)
        p = product(v, x)
        padded = [jnp.zeros((sweeps, v.shape[1]), jnp.float32), v, jnp.zeros((128 - 3 * sweeps, v.shape[1]), jnp.float32)]
        g = lax.dot_general(
            v, jnp.concatenate(padded, 0), (((1,), (1,)), ((), ())), precision=HIGHEST, preferred_element_type=jnp.float32
        )
        g = jnp.concatenate([g[:sweeps], pltpu.roll(g[sweeps:], 128 - sweeps, 1)], 0)
        return [p[:, h * 128 : (h + 1) * 128] for h in range(parts)] + [g]

    def project_own(first_chunk, count):
        b = first_chunk // per_block
        tile = jnp.concatenate([sets[first_chunk + i] for i in range(count)], 1)
        terms = project(tile, first_chunk * chunk, b, x_ref[first_chunk * chunk : (first_chunk + count) * chunk])
        for h, term in enumerate(terms):
            own[h, b * sweeps : (b + 2) * sweeps] += term

    groups = blocks + 1
    seam, other = (groups - 2) * sweeps, (2 * groups - 3) * sweeps
    below_end = other + (groups - 1) * sweeps

    def down():
        return remote(own.at[:, sweeps:], chain.at[:, : seam + sweeps], row_send.at[0], row_recv.at[0], row=below)

    def up():
        source = own.at[:, : (groups - 1) * sweeps]
        return remote(source, chain.at[:, other:below_end], row_send.at[1], row_recv.at[1], row=above)

    def tail_down():
        return remote(x_ref.at[rows - B :], tails.at[0], tail_send.at[0], tail_recv.at[0], row=below)

    def tail_up():
        return remote(x_ref.at[rows - B :], tails.at[1], tail_send.at[1], tail_recv.at[1], row=above)

    def to_rows():
        @pl.when(has_below)
        def _():
            down().start()

        @pl.when(has_above)
        def _():
            up().start()

    loads[2].wait()

    @pl.when(has_below)
    def _():
        tail_down().start()

    @pl.when(has_above)
    def _():
        tail_up().start()

    def answered(peer):
        @pl.when(peer > col)
        def _():
            arrived(peer)
            block_to(peer).start()

        if 2 <= peer < end:

            @pl.when((col == 1) & apart)
            def _():
                passed_on(peer).start()

    for peer in range(head):
        answered(peer)
        if peer % per_block == per_block - 1:

            @pl.when(peer - per_block + 1 >= col)
            def _():
                project_own(peer - per_block + 1, per_block)

    for first in range(0, head, per_block):
        for peer in range(first, first + per_block):

            @pl.when(peer < col)
            def _():
                arrived(peer)

        @pl.when(first < col)
        def _():
            project_own(first, per_block)

    to_rows()
    for which in range(per_block):
        peer = head + which
        answered(peer)

        @pl.when(peer < col)
        def _():
            arrived(peer)

        @pl.when((peer != col) & ((col > 0) if peer == end else (col >= 0)))
        def _():
            asides(which, col, start)

    chain[:, seam + sweeps : other] = own[:, sweeps : (groups - 1) * sweeps]
    chain[:, below_end:] = jnp.zeros((parts + 1, chain_rows - below_end, 128), jnp.float32)

    @pl.when(jnp.logical_not(has_above))
    def _():
        chain[:, : seam + sweeps] = jnp.zeros((parts + 1, seam + sweeps, 128), jnp.float32)
        side[0] = jnp.zeros(side.shape[1:], jnp.float32)
        tails[0] = jnp.zeros_like(tails[0])

    @pl.when(jnp.logical_not(has_below))
    def _():
        chain[:, other:below_end] = jnp.zeros((parts + 1, below_end - other, 128), jnp.float32)
        side[1] = jnp.zeros(side.shape[1:], jnp.float32)
        tails[1] = jnp.zeros_like(tails[1])

    @pl.when(has_above)
    def _():
        tail_down().wait_recv()
        down().wait_recv()
        for which in range(per_block):
            aside(which, col, False).wait_recv()

    @pl.when(has_below)
    def _():
        tail_up().wait_recv()
        up().wait_recv()
        for which in range(per_block):
            aside(which, col, True).wait_recv()

    last = rows - B
    mine = project(jnp.concatenate([sets[head + i] for i in range(per_block)], 1), last, blocks - 1, x_ref[last:])
    theirs = [
        project(jnp.concatenate([side[slot, i] for i in range(per_block)], 1), last, blocks - 1, tails[slot]) for slot in range(2)
    ]
    for h in range(parts + 1):
        chain[h, seam : seam + sweeps] += own[h, :sweeps] + theirs[0][h][sweeps:]
        chain[h, seam - sweeps : seam] += theirs[0][h][:sweeps]
        chain[h, other - sweeps : other] += mine[h][:sweeps]
        chain[h, other : other + sweeps] += own[h, (groups - 1) * sweeps :] + mine[h][sweeps:]
        chain[h, below_end - sweeps : below_end] += theirs[1][h][:sweeps]

    own_at = groups - 2
    total = chain_rows // sweeps
    place = lax.broadcasted_iota(jnp.int32, (total, 1), 0)
    first = jnp.where(has_above, 0, own_at + 1)
    stop = jnp.where(has_below, own_at + 2 * groups - 2, own_at + groups - 1)
    valid = (place >= first) & (place < stop)
    most = coef_ref.shape[1] // sweeps
    solved = []
    for s in range(sweeps):
        gram = chain[parts, pl.ds(s, total, stride=sweeps), :]
        acc = jnp.concatenate([chain[h, pl.ds(s, total, stride=sweeps), :] for h in range(parts)], 1)
        for p in range(s):
            before, here, after = solved[p]
            acc -= gram[:, sweeps + p : sweeps + p + 1] * here
            acc -= gram[:, p : p + 1] * before
            acc -= gram[:, 2 * sweeps + p : 2 * sweeps + p + 1] * after
        square = gram[:, sweeps + s : sweeps + s + 1]
        tau = jnp.where(valid, 2.0 / jnp.where(valid, square, 1.0), 0.0)
        here = tau * acc
        solved.append((pltpu.roll(here, 1, 0), here, pltpu.roll(here, total - 1, 0)))
        kept = pltpu.roll(here, total - own_at, 0)[:most]
        for h in range(parts):
            coef_ref[h, pl.ds(s, most, stride=sweeps), :] = kept[:, h * 128 : (h + 1) * 128]
    for i in range(n_col):
        sets_ref[i] = sets[i]

    for peer in range(n_col):

        @pl.when((peer != col) & (to_first if peer == 0 else (col >= 0)))
        def _():
            block_to(peer).wait_send()

        if 2 <= peer < end:

            @pl.when((col == 1) & apart)
            def _():
                passed_on(peer).wait_send()

    for which in range(per_block):

        @pl.when((col > 0) if which == per_block - 1 else (col >= 0))
        def _():
            asides(which, col, sent_off)

    @pl.when(col == end)
    def _():
        asides(per_block - 1, 0, sent_off, 2 * per_block)

    @pl.when(has_below)
    def _():
        tail_down().wait_send()
        down().wait_send()

    @pl.when(has_above)
    def _():
        tail_up().wait_send()
        up().wait_send()


def update_kernel(off_ref, sets_ref, coef_ref, x_ref, out_hbm, out, out_sem):
    count, sweeps, chunk = sets_ref.shape
    per_block = B // chunk
    off = off_ref[:, :1]
    steps = out.shape[0]
    blocks = count // per_block // steps

    def write(step):
        return pltpu.make_async_copy(out.at[step], out_hbm.at[pl.ds(step * blocks * B, blocks * B)], out_sem.at[step])

    for step in range(steps):
        for i in range(blocks):
            b = step * blocks + i
            tile = jnp.concatenate([sets_ref[b * per_block + j] for j in range(per_block)], 1)
            v_high, v_low = halves(masked_sets(tile, off, b * B, b))
            z = [coef_ref[h, b * sweeps : (b + 2) * sweeps, :] for h in range(coef_ref.shape[0])]
            z_high, z_low = halves(jnp.concatenate(z, 1))
            out[step, i * B : (i + 1) * B] = x_ref[b * B : (b + 1) * B] - lax.dot_general(
                jnp.concatenate([v_high, v_low, v_high], 0),
                jnp.concatenate([z_high, z_high, z_low], 0),
                (((0,), (0,)), ((), ())),
                preferred_element_type=jnp.float32,
            )
        write(step).start()
    for step in range(steps):
        write(step).wait()


def body(n_col, n_row, eigvec, reflectors, offsets):
    rows, cols = eigvec.shape
    sweeps, chunk = reflectors.shape
    groups = rows // B + 1
    total, most = (-(-count // 8) * 8 for count in (3 * groups - 3, groups))
    vmem, hbm = pl.BlockSpec(memory_space=pltpu.VMEM), pl.BlockSpec(memory_space=pl.ANY)
    parts, per_block = cols // 128, B // chunk
    dma, f32 = pltpu.SemaphoreType.DMA, jnp.float32
    held = pl.pallas_call(
        functools.partial(coupling_kernel, n_col, n_row),
        out_shape=(
            pltpu.VMEM((n_col, sweeps, chunk), f32),
            pltpu.VMEM((parts, most * sweeps, 128), f32),
            pltpu.VMEM((sweeps, 128), jnp.int32),
            pltpu.VMEM(eigvec.shape, f32),
        ),
        in_specs=[hbm, hbm, hbm],
        out_specs=(vmem, vmem, vmem, vmem),
        scratch_shapes=[
            pltpu.VMEM((n_col, sweeps, chunk), f32),
            pltpu.VMEM((parts + 1, groups * sweeps, 128), f32),
            pltpu.VMEM((parts + 1, total * sweeps, 128), f32),
            pltpu.VMEM((2, per_block, sweeps, chunk), f32),
            pltpu.VMEM((2, B, cols), f32),
            pltpu.SMEM(offsets.shape, jnp.int32),
            dma((n_col,)),
            dma((n_col,)),
            dma((n_col,)),
            dma((2,)),
            dma((2,)),
            dma((4 * per_block,)),
            dma((2 * per_block,)),
            dma((2,)),
            dma((2,)),
            dma((3,)),
        ],
        compiler_params=pltpu.CompilerParams(collective_id=0, has_side_effects=True),
        name="coupling",
    )(offsets, reflectors, eigvec)
    sets, coef, off, x = (pltpu.with_memory_space_constraint(array, pltpu.VMEM) for array in held)
    steps = 4
    return pl.pallas_call(
        update_kernel,
        out_shape=jax.ShapeDtypeStruct(eigvec.shape, f32),
        in_specs=[vmem, vmem, vmem, vmem],
        out_specs=hbm,
        scratch_shapes=[pltpu.VMEM((steps, rows // steps, cols), f32), dma((steps,))],
        name="update",
    )(off, sets, coef, x)


def solution(mesh):
    in_specs = (P(("grp", "row"), "col"), P(None, ("grp", "row", "col")), P("grp"))
    out_specs = P(("grp", "row"), "col")
    step = functools.partial(body, mesh.shape["col"], mesh.shape["row"])
    return jax.shard_map(step, mesh=mesh, in_specs=in_specs, out_specs=out_specs, check_vma=False)
```

```python
import functools

import jax
import jax.numpy as jnp
from jax import lax
from jax.experimental import pallas as pl
from jax.experimental.pallas import tpu as pltpu
from jax.sharding import PartitionSpec as P

B = 256
MESH = pl.DeviceIdType.MESH
HIGHEST = lax.Precision.HIGHEST


def masked_sets(tile, off, first_row, group):
    row = first_row + lax.broadcasted_iota(jnp.int32, tile.shape, 1) - group * B
    tile = jnp.where(row == off, 1.0, tile)
    before = row < off
    return jnp.concatenate([jnp.where(before, tile, 0.0), jnp.where(before, 0.0, tile)], 0)


def offset_column(off_ref, sweeps):
    which = lax.broadcasted_iota(jnp.int32, (sweeps, 1), 0)
    off = jnp.zeros((sweeps, 1), jnp.int32)
    for s in range(sweeps):
        off = jnp.where(which == s, off_ref[s], off)
    return off


def halves(x):
    high = x.astype(jnp.bfloat16)
    return high, (x - high.astype(jnp.float32)).astype(jnp.bfloat16)


def product(v, x):
    count = v.shape[0]
    v_high, v_low = halves(v)
    x_high, x_low = halves(x)
    both = jnp.dot(jnp.concatenate([v_high, v_low], 0), x_high, preferred_element_type=jnp.float32)
    return both[:count] + both[count:] + jnp.dot(v_high, x_low, preferred_element_type=jnp.float32)


def coupling_kernel(
    n_col, n_row, off_hbm, refl_hbm, eig_hbm, sets_ref, coef_ref, off_ref, x_ref,
    sets, own, chain, side, tails, off_smem, sent, passed, recv, row_send, row_recv, side_send, side_recv, tail_send, tail_recv, loaded,
):
    sweeps, chunk = refl_hbm.shape
    rows, cols = eig_hbm.shape
    blocks, parts = rows // B, cols // 128
    per_block = B // chunk
    col = lax.axis_index("col")
    row = lax.axis_index("row")
    has_above, has_below = row > 0, row < n_row - 1
    end, head = n_col - 1, n_col - per_block
    apart = (row == 0) & (lax.axis_index("grp") == 0)

    loads = [
        pltpu.make_async_copy(refl_hbm, sets.at[col], loaded.at[0]),
        pltpu.make_async_copy(off_hbm, off_smem, loaded.at[1]),
        pltpu.make_async_copy(eig_hbm, x_ref, loaded.at[2]),
    ]
    for load in loads:
        load.start()

    barrier = pltpu.get_barrier_semaphore()

    def greet(axis, peer):
        pl.semaphore_signal(barrier, inc=1, device_id={axis: peer}, device_id_type=MESH)

    @pl.when(has_above)
    def _():
        greet("row", row - 1)

    @pl.when(has_below)
    def _():
        greet("row", row + 1)

    @pl.when(col == 0)
    def _():
        greet("col", 1)

    @pl.when((col == 1) & apart)
    def _():
        greet("col", 2)

    peers = jnp.where(has_above, 1, 0) + jnp.where(has_below, 1, 0) + jnp.where(col == 0, 0, 1) + jnp.where(col == end, 1, 0)
    pl.semaphore_wait(barrier, peers)

    @pl.when(col == 0)
    def _():
        greet("col", end)

    @pl.when(((col >= 2) | ((col == 1) & jnp.logical_not(apart))) & (col < end))
    def _():
        greet("col", col + 1)

    def remote(source, target, send_sem, recv_sem, **device):
        return pltpu.make_async_remote_copy(
            src_ref=source, dst_ref=target, send_sem=send_sem, recv_sem=recv_sem, device_id=device, device_id_type=MESH
        )

    def block_to(peer):
        return remote(sets.at[col], sets.at[col], sent.at[peer], recv.at[col], col=peer)

    def passed_on(index):
        return remote(sets.at[index], sets.at[index], passed.at[index], recv.at[index], col=0)

    def arrived(index):
        remote(sets.at[index], sets.at[index], sent.at[index], recv.at[index], col=index).wait_recv()

    above, below = jnp.maximum(row - 1, 0), jnp.minimum(row + 1, n_row - 1)

    def aside(which, peer_col, upward, extra=0):
        slot, peer = (1, above) if upward else (0, below)
        target, index = side.at[slot, which], slot * per_block + which
        return remote(sets.at[head + which], target, side_send.at[index + extra], side_recv.at[index], row=peer, col=peer_col)

    def asides(which, peer_col, act, extra=0):
        @pl.when(has_below)
        def _():
            act(aside(which, peer_col, False, extra))

        @pl.when(has_above)
        def _():
            act(aside(which, peer_col, True, extra))

    def start(copy):
        copy.start()

    def sent_off(copy):
        copy.wait_send()

    loads[0].wait()

    relay = (col == 1) & apart
    to_first = (col == 1) | (col == end) | ((col > 0) & jnp.logical_not(apart))

    @pl.when(to_first)
    def _():
        block_to(0).start()

    @pl.when(relay)
    def _():
        for peer in range(2, end):
            arrived(peer)
            passed_on(peer).start()
            block_to(peer).start()

    @pl.when(col == end)
    def _():
        asides(per_block - 1, 0, start, 2 * per_block)

    for peer in range(1, end):

        @pl.when(peer < col)
        def _():
            block_to(peer).start()

    for which in range(per_block):

        @pl.when(col == head + which)
        def _():
            asides(which, col, start)

    loads[1].wait()
    off = offset_column(off_smem, sweeps)
    off_ref[...] = jnp.broadcast_to(off, off_ref.shape)
    own[...] = jnp.zeros_like(own)
    chain_rows = chain.shape[1]

    def project(tile, first, b, x):
        v = masked_sets(tile, off, first, b)
        p = product(v, x)
        padded = [jnp.zeros((sweeps, v.shape[1]), jnp.float32), v, jnp.zeros((128 - 3 * sweeps, v.shape[1]), jnp.float32)]
        g = lax.dot_general(
            v, jnp.concatenate(padded, 0), (((1,), (1,)), ((), ())), precision=HIGHEST, preferred_element_type=jnp.float32
        )
        g = jnp.concatenate([g[:sweeps], pltpu.roll(g[sweeps:], 128 - sweeps, 1)], 0)
        return [p[:, h * 128 : (h + 1) * 128] for h in range(parts)] + [g]

    def project_own(first_chunk, count):
        b = first_chunk // per_block
        tile = jnp.concatenate([sets[first_chunk + i] for i in range(count)], 1)
        terms = project(tile, first_chunk * chunk, b, x_ref[first_chunk * chunk : (first_chunk + count) * chunk])
        for h, term in enumerate(terms):
            own[h, b * sweeps : (b + 2) * sweeps] += term

    groups = blocks + 1
    seam, other = (groups - 2) * sweeps, (2 * groups - 3) * sweeps
    below_end = other + (groups - 1) * sweeps

    def down():
        return remote(own.at[:, sweeps:], chain.at[:, : seam + sweeps], row_send.at[0], row_recv.at[0], row=below)

    def up():
        source = own.at[:, : (groups - 1) * sweeps]
        return remote(source, chain.at[:, other:below_end], row_send.at[1], row_recv.at[1], row=above)

    def tail_down():
        return remote(x_ref.at[rows - B :], tails.at[0], tail_send.at[0], tail_recv.at[0], row=below)

    def tail_up():
        return remote(x_ref.at[rows - B :], tails.at[1], tail_send.at[1], tail_recv.at[1], row=above)

    def to_rows():
        @pl.when(has_below)
        def _():
            down().start()

        @pl.when(has_above)
        def _():
            up().start()

    loads[2].wait()

    @pl.when(has_below)
    def _():
        tail_down().start()

    @pl.when(has_above)
    def _():
        tail_up().start()

    def answered(peer):
        @pl.when((peer > col) & (jnp.logical_not(relay) if 2 <= peer < end else (col >= 0)))
        def _():
            arrived(peer)
            block_to(peer).start()

    for peer in range(head):
        answered(peer)
        if peer % per_block == per_block - 1:

            @pl.when(peer - per_block + 1 >= col)
            def _():
                project_own(peer - per_block + 1, per_block)

    for first in range(0, head, per_block):
        for peer in range(first, first + per_block):

            @pl.when(peer < col)
            def _():
                arrived(peer)

        @pl.when(first < col)
        def _():
            project_own(first, per_block)

    to_rows()
    for which in range(per_block):
        peer = head + which
        answered(peer)

        @pl.when(peer < col)
        def _():
            arrived(peer)

        @pl.when((peer != col) & ((col > 0) if peer == end else (col >= 0)))
        def _():
            asides(which, col, start)

    chain[:, seam + sweeps : other] = own[:, sweeps : (groups - 1) * sweeps]
    chain[:, below_end:] = jnp.zeros((parts + 1, chain_rows - below_end, 128), jnp.float32)

    @pl.when(jnp.logical_not(has_above))
    def _():
        chain[:, : seam + sweeps] = jnp.zeros((parts + 1, seam + sweeps, 128), jnp.float32)
        side[0] = jnp.zeros(side.shape[1:], jnp.float32)
        tails[0] = jnp.zeros_like(tails[0])

    @pl.when(jnp.logical_not(has_below))
    def _():
        chain[:, other:below_end] = jnp.zeros((parts + 1, below_end - other, 128), jnp.float32)
        side[1] = jnp.zeros(side.shape[1:], jnp.float32)
        tails[1] = jnp.zeros_like(tails[1])

    @pl.when(has_above)
    def _():
        tail_down().wait_recv()
        down().wait_recv()
        for which in range(per_block):
            aside(which, col, False).wait_recv()

    @pl.when(has_below)
    def _():
        tail_up().wait_recv()
        up().wait_recv()
        for which in range(per_block):
            aside(which, col, True).wait_recv()

    last = rows - B
    mine = project(jnp.concatenate([sets[head + i] for i in range(per_block)], 1), last, blocks - 1, x_ref[last:])
    theirs = [
        project(jnp.concatenate([side[slot, i] for i in range(per_block)], 1), last, blocks - 1, tails[slot]) for slot in range(2)
    ]
    for h in range(parts + 1):
        chain[h, seam : seam + sweeps] += own[h, :sweeps] + theirs[0][h][sweeps:]
        chain[h, seam - sweeps : seam] += theirs[0][h][:sweeps]
        chain[h, other - sweeps : other] += mine[h][:sweeps]
        chain[h, other : other + sweeps] += own[h, (groups - 1) * sweeps :] + mine[h][sweeps:]
        chain[h, below_end - sweeps : below_end] += theirs[1][h][:sweeps]

    own_at = groups - 2
    total = chain_rows // sweeps
    place = lax.broadcasted_iota(jnp.int32, (total, 1), 0)
    first = jnp.where(has_above, 0, own_at + 1)
    stop = jnp.where(has_below, own_at + 2 * groups - 2, own_at + groups - 1)
    valid = (place >= first) & (place < stop)
    most = coef_ref.shape[1] // sweeps
    solved = []
    for s in range(sweeps):
        gram = chain[parts, pl.ds(s, total, stride=sweeps), :]
        acc = jnp.concatenate([chain[h, pl.ds(s, total, stride=sweeps), :] for h in range(parts)], 1)
        for p in range(s):
            before, here, after = solved[p]
            acc -= gram[:, sweeps + p : sweeps + p + 1] * here
            acc -= gram[:, p : p + 1] * before
            acc -= gram[:, 2 * sweeps + p : 2 * sweeps + p + 1] * after
        square = gram[:, sweeps + s : sweeps + s + 1]
        tau = jnp.where(valid, 2.0 / jnp.where(valid, square, 1.0), 0.0)
        here = tau * acc
        solved.append((pltpu.roll(here, 1, 0), here, pltpu.roll(here, total - 1, 0)))
        kept = pltpu.roll(here, total - own_at, 0)[:most]
        for h in range(parts):
            coef_ref[h, pl.ds(s, most, stride=sweeps), :] = kept[:, h * 128 : (h + 1) * 128]
    for i in range(n_col):
        sets_ref[i] = sets[i]

    for peer in range(n_col):

        @pl.when((peer != col) & (to_first if peer == 0 else (col >= 0)))
        def _():
            block_to(peer).wait_send()

        if 2 <= peer < end:

            @pl.when(relay)
            def _():
                passed_on(peer).wait_send()

    for which in range(per_block):

        @pl.when((col > 0) if which == per_block - 1 else (col >= 0))
        def _():
            asides(which, col, sent_off)

    @pl.when(col == end)
    def _():
        asides(per_block - 1, 0, sent_off, 2 * per_block)

    @pl.when(has_below)
    def _():
        tail_down().wait_send()
        down().wait_send()

    @pl.when(has_above)
    def _():
        tail_up().wait_send()
        up().wait_send()


def update_kernel(off_ref, sets_ref, coef_ref, x_ref, out_hbm, out, out_sem):
    count, sweeps, chunk = sets_ref.shape
    per_block = B // chunk
    off = off_ref[:, :1]
    steps = out.shape[0]
    blocks = count // per_block // steps

    def write(step):
        return pltpu.make_async_copy(out.at[step], out_hbm.at[pl.ds(step * blocks * B, blocks * B)], out_sem.at[step])

    for step in range(steps):
        for i in range(blocks):
            b = step * blocks + i
            tile = jnp.concatenate([sets_ref[b * per_block + j] for j in range(per_block)], 1)
            v_high, v_low = halves(masked_sets(tile, off, b * B, b))
            z = [coef_ref[h, b * sweeps : (b + 2) * sweeps, :] for h in range(coef_ref.shape[0])]
            z_high, z_low = halves(jnp.concatenate(z, 1))
            out[step, i * B : (i + 1) * B] = x_ref[b * B : (b + 1) * B] - lax.dot_general(
                jnp.concatenate([v_high, v_low, v_high], 0),
                jnp.concatenate([z_high, z_high, z_low], 0),
                (((0,), (0,)), ((), ())),
                preferred_element_type=jnp.float32,
            )
        write(step).start()
    for step in range(steps):
        write(step).wait()


def body(n_col, n_row, eigvec, reflectors, offsets):
    rows, cols = eigvec.shape
    sweeps, chunk = reflectors.shape
    groups = rows // B + 1
    total, most = (-(-count // 8) * 8 for count in (3 * groups - 3, groups))
    vmem, hbm = pl.BlockSpec(memory_space=pltpu.VMEM), pl.BlockSpec(memory_space=pl.ANY)
    parts, per_block = cols // 128, B // chunk
    dma, f32 = pltpu.SemaphoreType.DMA, jnp.float32
    held = pl.pallas_call(
        functools.partial(coupling_kernel, n_col, n_row),
        out_shape=(
            pltpu.VMEM((n_col, sweeps, chunk), f32),
            pltpu.VMEM((parts, most * sweeps, 128), f32),
            pltpu.VMEM((sweeps, 128), jnp.int32),
            pltpu.VMEM(eigvec.shape, f32),
        ),
        in_specs=[hbm, hbm, hbm],
        out_specs=(vmem, vmem, vmem, vmem),
        scratch_shapes=[
            pltpu.VMEM((n_col, sweeps, chunk), f32),
            pltpu.VMEM((parts + 1, groups * sweeps, 128), f32),
            pltpu.VMEM((parts + 1, total * sweeps, 128), f32),
            pltpu.VMEM((2, per_block, sweeps, chunk), f32),
            pltpu.VMEM((2, B, cols), f32),
            pltpu.SMEM(offsets.shape, jnp.int32),
            dma((n_col,)),
            dma((n_col,)),
            dma((n_col,)),
            dma((2,)),
            dma((2,)),
            dma((4 * per_block,)),
            dma((2 * per_block,)),
            dma((2,)),
            dma((2,)),
            dma((3,)),
        ],
        compiler_params=pltpu.CompilerParams(collective_id=0, has_side_effects=True),
        name="coupling",
    )(offsets, reflectors, eigvec)
    sets, coef, off, x = (pltpu.with_memory_space_constraint(array, pltpu.VMEM) for array in held)
    steps = 4
    return pl.pallas_call(
        update_kernel,
        out_shape=jax.ShapeDtypeStruct(eigvec.shape, f32),
        in_specs=[vmem, vmem, vmem, vmem],
        out_specs=hbm,
        scratch_shapes=[pltpu.VMEM((steps, rows // steps, cols), f32), dma((steps,))],
        name="update",
    )(off, sets, coef, x)


def solution(mesh):
    in_specs = (P(("grp", "row"), "col"), P(None, ("grp", "row", "col")), P("grp"))
    out_specs = P(("grp", "row"), "col")
    step = functools.partial(body, mesh.shape["col"], mesh.shape["row"])
    return jax.shard_map(step, mesh=mesh, in_specs=in_specs, out_specs=out_specs, check_vma=False)
```

```python
import functools

import jax
import jax.numpy as jnp
from jax import lax
from jax.experimental import pallas as pl
from jax.experimental.pallas import tpu as pltpu
from jax.sharding import PartitionSpec as P

B = 256
MESH = pl.DeviceIdType.MESH
HIGHEST = lax.Precision.HIGHEST


def masked_sets(tile, off, first_row, group):
    row = first_row + lax.broadcasted_iota(jnp.int32, tile.shape, 1) - group * B
    tile = jnp.where(row == off, 1.0, tile)
    before = row < off
    return jnp.concatenate([jnp.where(before, tile, 0.0), jnp.where(before, 0.0, tile)], 0)


def offset_column(off_ref, sweeps):
    which = lax.broadcasted_iota(jnp.int32, (sweeps, 1), 0)
    off = jnp.zeros((sweeps, 1), jnp.int32)
    for s in range(sweeps):
        off = jnp.where(which == s, off_ref[s], off)
    return off


def halves(x):
    high = x.astype(jnp.bfloat16)
    return high, (x - high.astype(jnp.float32)).astype(jnp.bfloat16)


def product(v, x):
    count = v.shape[0]
    v_high, v_low = halves(v)
    x_high, x_low = halves(x)
    both = jnp.dot(jnp.concatenate([v_high, v_low], 0), x_high, preferred_element_type=jnp.float32)
    return both[:count] + both[count:] + jnp.dot(v_high, x_low, preferred_element_type=jnp.float32)


def coupling_kernel(
    n_col, n_row, off_hbm, refl_hbm, eig_hbm, sets_ref, coef_ref, off_ref, x_ref,
    sets, own, chain, side, tails, off_smem, sent, passed, recv, row_send, row_recv, side_send, side_recv, tail_send, tail_recv, loaded,
):
    sweeps, chunk = refl_hbm.shape
    rows, cols = eig_hbm.shape
    blocks, parts = rows // B, cols // 128
    per_block = B // chunk
    col = lax.axis_index("col")
    row = lax.axis_index("row")
    has_above, has_below = row > 0, row < n_row - 1
    end, head = n_col - 1, n_col - per_block
    apart = (row == 0) & (lax.axis_index("grp") == 0)

    loads = [
        pltpu.make_async_copy(refl_hbm, sets.at[col], loaded.at[0]),
        pltpu.make_async_copy(off_hbm, off_smem, loaded.at[1]),
        pltpu.make_async_copy(eig_hbm, x_ref, loaded.at[2]),
    ]
    for load in loads:
        load.start()

    barrier = pltpu.get_barrier_semaphore()

    def greet(axis, peer):
        pl.semaphore_signal(barrier, inc=1, device_id={axis: peer}, device_id_type=MESH)

    @pl.when(has_above)
    def _():
        greet("row", row - 1)

    @pl.when(has_below)
    def _():
        greet("row", row + 1)

    @pl.when((col == 0) & jnp.logical_not(apart))
    def _():
        greet("col", 1)

    @pl.when((col == 1) & apart)
    def _():
        greet("col", 2)

    peers = jnp.where(has_above, 1, 0) + jnp.where(has_below, 1, 0) + jnp.where(col == 0, 0, 1) + jnp.where(col == end, 1, 0)
    pl.semaphore_wait(barrier, peers)

    @pl.when((col == 0) & apart)
    def _():
        greet("col", 1)

    @pl.when(col == 0)
    def _():
        greet("col", end)

    @pl.when(((col >= 2) | ((col == 1) & jnp.logical_not(apart))) & (col < end))
    def _():
        greet("col", col + 1)

    def remote(source, target, send_sem, recv_sem, **device):
        return pltpu.make_async_remote_copy(
            src_ref=source, dst_ref=target, send_sem=send_sem, recv_sem=recv_sem, device_id=device, device_id_type=MESH
        )

    def block_to(peer):
        return remote(sets.at[col], sets.at[col], sent.at[peer], recv.at[col], col=peer)

    def passed_on(index):
        return remote(sets.at[index], sets.at[index], passed.at[index], recv.at[index], col=0)

    def arrived(index):
        remote(sets.at[index], sets.at[index], sent.at[index], recv.at[index], col=index).wait_recv()

    above, below = jnp.maximum(row - 1, 0), jnp.minimum(row + 1, n_row - 1)

    def aside(which, peer_col, upward, extra=0):
        slot, peer = (1, above) if upward else (0, below)
        target, index = side.at[slot, which], slot * per_block + which
        return remote(sets.at[head + which], target, side_send.at[index + extra], side_recv.at[index], row=peer, col=peer_col)

    def asides(which, peer_col, act, extra=0):
        @pl.when(has_below)
        def _():
            act(aside(which, peer_col, False, extra))

        @pl.when(has_above)
        def _():
            act(aside(which, peer_col, True, extra))

    def start(copy):
        copy.start()

    def sent_off(copy):
        copy.wait_send()

    loads[0].wait()

    relay, served = (col == 1) & apart, (col == 0) & apart

    def forwards(which):
        return col > 0 if which == per_block - 1 else jnp.logical_not(served)

    to_first = (col == 1) | (col == end) | ((col > 0) & jnp.logical_not(apart))

    @pl.when(to_first)
    def _():
        block_to(0).start()

    @pl.when(relay)
    def _():
        for peer in range(2, head):
            arrived(peer)
            passed_on(peer).start()
        for peer in range(2, head):
            block_to(peer).start()
        for which in range(per_block - 1):
            arrived(head + which)
            passed_on(head + which).start()
            asides(which, 0, start, 2 * per_block)
            block_to(head + which).start()

    @pl.when(col == end)
    def _():
        asides(per_block - 1, 0, start, 2 * per_block)

    for peer in range(1, end):

        @pl.when(peer < col)
        def _():
            block_to(peer).start()

    for which in range(per_block):

        @pl.when(col == head + which)
        def _():
            asides(which, col, start)

    loads[1].wait()
    off = offset_column(off_smem, sweeps)
    off_ref[...] = jnp.broadcast_to(off, off_ref.shape)
    own[...] = jnp.zeros_like(own)
    chain_rows = chain.shape[1]

    def project(tile, first, b, x):
        v = masked_sets(tile, off, first, b)
        p = product(v, x)
        padded = [jnp.zeros((sweeps, v.shape[1]), jnp.float32), v, jnp.zeros((128 - 3 * sweeps, v.shape[1]), jnp.float32)]
        g = lax.dot_general(
            v, jnp.concatenate(padded, 0), (((1,), (1,)), ((), ())), precision=HIGHEST, preferred_element_type=jnp.float32
        )
        g = jnp.concatenate([g[:sweeps], pltpu.roll(g[sweeps:], 128 - sweeps, 1)], 0)
        return [p[:, h * 128 : (h + 1) * 128] for h in range(parts)] + [g]

    def project_own(first_chunk, count):
        b = first_chunk // per_block
        tile = jnp.concatenate([sets[first_chunk + i] for i in range(count)], 1)
        terms = project(tile, first_chunk * chunk, b, x_ref[first_chunk * chunk : (first_chunk + count) * chunk])
        for h, term in enumerate(terms):
            own[h, b * sweeps : (b + 2) * sweeps] += term

    groups = blocks + 1
    seam, other = (groups - 2) * sweeps, (2 * groups - 3) * sweeps
    below_end = other + (groups - 1) * sweeps

    def down():
        return remote(own.at[:, sweeps:], chain.at[:, : seam + sweeps], row_send.at[0], row_recv.at[0], row=below)

    def up():
        source = own.at[:, : (groups - 1) * sweeps]
        return remote(source, chain.at[:, other:below_end], row_send.at[1], row_recv.at[1], row=above)

    def tail_down():
        return remote(x_ref.at[rows - B :], tails.at[0], tail_send.at[0], tail_recv.at[0], row=below)

    def tail_up():
        return remote(x_ref.at[rows - B :], tails.at[1], tail_send.at[1], tail_recv.at[1], row=above)

    def to_rows():
        @pl.when(has_below)
        def _():
            down().start()

        @pl.when(has_above)
        def _():
            up().start()

    loads[2].wait()

    @pl.when(has_below)
    def _():
        tail_down().start()

    @pl.when(has_above)
    def _():
        tail_up().start()

    def answered(peer):
        @pl.when((peer > col) & (jnp.logical_not(relay) if 2 <= peer < end else (col >= 0)))
        def _():
            arrived(peer)

        def answer():
            block_to(peer).start()

        now = (peer > col) & (jnp.logical_not(relay) if 2 <= peer < end else (col >= 0))
        if 2 <= peer < head:
            now &= jnp.logical_not(served)
        pl.when(now)(answer)

    def early_sent():
        for peer in range(head):

            @pl.when((peer != col) & (to_first if peer == 0 else (col >= 0)))
            def _():
                block_to(peer).wait_send()

        @pl.when(relay)
        def _():
            for peer in range(2, end):
                passed_on(peer).wait_send()
            for which in range(per_block - 1):
                asides(which, 0, sent_off, 2 * per_block)

        @pl.when(has_below)
        def _():
            tail_down().wait_send()

        @pl.when(has_above)
        def _():
            tail_up().wait_send()

    for peer in range(head):
        answered(peer)
        if peer % per_block == per_block - 1:

            @pl.when(peer - per_block + 1 >= col)
            def _():
                project_own(peer - per_block + 1, per_block)

    for first in range(0, head, per_block):
        for peer in range(first, first + per_block):

            @pl.when(peer < col)
            def _():
                arrived(peer)

        @pl.when(first < col)
        def _():
            project_own(first, per_block)

    to_rows()

    @pl.when(served)
    def _():
        for peer in range(2, head):
            block_to(peer).start()

    for which in range(per_block):
        if which == per_block - 1:
            early_sent()
        peer = head + which
        answered(peer)

        @pl.when(peer < col)
        def _():
            arrived(peer)

        @pl.when((peer != col) & forwards(which))
        def _():
            asides(which, col, start)

    chain[:, seam + sweeps : other] = own[:, sweeps : (groups - 1) * sweeps]
    chain[:, below_end:] = jnp.zeros((parts + 1, chain_rows - below_end, 128), jnp.float32)

    @pl.when(jnp.logical_not(has_above))
    def _():
        chain[:, : seam + sweeps] = jnp.zeros((parts + 1, seam + sweeps, 128), jnp.float32)
        side[0] = jnp.zeros(side.shape[1:], jnp.float32)
        tails[0] = jnp.zeros_like(tails[0])

    @pl.when(jnp.logical_not(has_below))
    def _():
        chain[:, other:below_end] = jnp.zeros((parts + 1, below_end - other, 128), jnp.float32)
        side[1] = jnp.zeros(side.shape[1:], jnp.float32)
        tails[1] = jnp.zeros_like(tails[1])

    @pl.when(has_above)
    def _():
        tail_down().wait_recv()
        down().wait_recv()
        for which in range(per_block):
            aside(which, col, False).wait_recv()

    @pl.when(has_below)
    def _():
        tail_up().wait_recv()
        up().wait_recv()
        for which in range(per_block):
            aside(which, col, True).wait_recv()

    last = rows - B
    mine = project(jnp.concatenate([sets[head + i] for i in range(per_block)], 1), last, blocks - 1, x_ref[last:])
    theirs = [
        project(jnp.concatenate([side[slot, i] for i in range(per_block)], 1), last, blocks - 1, tails[slot]) for slot in range(2)
    ]
    for h in range(parts + 1):
        chain[h, seam : seam + sweeps] += own[h, :sweeps] + theirs[0][h][sweeps:]
        chain[h, seam - sweeps : seam] += theirs[0][h][:sweeps]
        chain[h, other - sweeps : other] += mine[h][:sweeps]
        chain[h, other : other + sweeps] += own[h, (groups - 1) * sweeps :] + mine[h][sweeps:]
        chain[h, below_end - sweeps : below_end] += theirs[1][h][:sweeps]

    own_at = groups - 2
    total = chain_rows // sweeps
    place = lax.broadcasted_iota(jnp.int32, (total, 1), 0)
    first = jnp.where(has_above, 0, own_at + 1)
    stop = jnp.where(has_below, own_at + 2 * groups - 2, own_at + groups - 1)
    valid = (place >= first) & (place < stop)
    most = coef_ref.shape[1] // sweeps
    solved = []
    for s in range(sweeps):
        gram = chain[parts, pl.ds(s, total, stride=sweeps), :]
        acc = jnp.concatenate([chain[h, pl.ds(s, total, stride=sweeps), :] for h in range(parts)], 1)
        for p in range(s):
            before, here, after = solved[p]
            acc -= gram[:, sweeps + p : sweeps + p + 1] * here
            acc -= gram[:, p : p + 1] * before
            acc -= gram[:, 2 * sweeps + p : 2 * sweeps + p + 1] * after
        square = gram[:, sweeps + s : sweeps + s + 1]
        tau = jnp.where(valid, 2.0 / jnp.where(valid, square, 1.0), 0.0)
        here = tau * acc
        solved.append((pltpu.roll(here, 1, 0), here, pltpu.roll(here, total - 1, 0)))
        kept = pltpu.roll(here, total - own_at, 0)[:most]
        for h in range(parts):
            coef_ref[h, pl.ds(s, most, stride=sweeps), :] = kept[:, h * 128 : (h + 1) * 128]
    for i in range(n_col):
        sets_ref[i] = sets[i]

    for peer in range(head, n_col):

        @pl.when(peer != col)
        def _():
            block_to(peer).wait_send()

    for which in range(per_block):

        @pl.when(forwards(which))
        def _():
            asides(which, col, sent_off)

    @pl.when(col == end)
    def _():
        asides(per_block - 1, 0, sent_off, 2 * per_block)

    @pl.when(has_below)
    def _():
        down().wait_send()

    @pl.when(has_above)
    def _():
        up().wait_send()


def update_kernel(off_ref, sets_ref, coef_ref, x_ref, out_hbm, out, out_sem):
    count, sweeps, chunk = sets_ref.shape
    per_block = B // chunk
    off = off_ref[:, :1]
    steps = out.shape[0]
    blocks = count // per_block // steps

    def write(step):
        return pltpu.make_async_copy(out.at[step], out_hbm.at[pl.ds(step * blocks * B, blocks * B)], out_sem.at[step])

    for step in range(steps):
        for i in range(blocks):
            b = step * blocks + i
            tile = jnp.concatenate([sets_ref[b * per_block + j] for j in range(per_block)], 1)
            v_high, v_low = halves(masked_sets(tile, off, b * B, b))
            z = [coef_ref[h, b * sweeps : (b + 2) * sweeps, :] for h in range(coef_ref.shape[0])]
            z_high, z_low = halves(jnp.concatenate(z, 1))
            out[step, i * B : (i + 1) * B] = x_ref[b * B : (b + 1) * B] - lax.dot_general(
                jnp.concatenate([v_high, v_low, v_high], 0),
                jnp.concatenate([z_high, z_high, z_low], 0),
                (((0,), (0,)), ((), ())),
                preferred_element_type=jnp.float32,
            )
        write(step).start()
    for step in range(steps):
        write(step).wait()


def body(n_col, n_row, eigvec, reflectors, offsets):
    rows, cols = eigvec.shape
    sweeps, chunk = reflectors.shape
    groups = rows // B + 1
    total, most = (-(-count // 8) * 8 for count in (3 * groups - 3, groups))
    vmem, hbm = pl.BlockSpec(memory_space=pltpu.VMEM), pl.BlockSpec(memory_space=pl.ANY)
    parts, per_block = cols // 128, B // chunk
    dma, f32 = pltpu.SemaphoreType.DMA, jnp.float32
    held = pl.pallas_call(
        functools.partial(coupling_kernel, n_col, n_row),
        out_shape=(
            pltpu.VMEM((n_col, sweeps, chunk), f32),
            pltpu.VMEM((parts, most * sweeps, 128), f32),
            pltpu.VMEM((sweeps, 128), jnp.int32),
            pltpu.VMEM(eigvec.shape, f32),
        ),
        in_specs=[hbm, hbm, hbm],
        out_specs=(vmem, vmem, vmem, vmem),
        scratch_shapes=[
            pltpu.VMEM((n_col, sweeps, chunk), f32),
            pltpu.VMEM((parts + 1, groups * sweeps, 128), f32),
            pltpu.VMEM((parts + 1, total * sweeps, 128), f32),
            pltpu.VMEM((2, per_block, sweeps, chunk), f32),
            pltpu.VMEM((2, B, cols), f32),
            pltpu.SMEM(offsets.shape, jnp.int32),
            dma((n_col,)),
            dma((n_col,)),
            dma((n_col,)),
            dma((2,)),
            dma((2,)),
            dma((4 * per_block,)),
            dma((2 * per_block,)),
            dma((2,)),
            dma((2,)),
            dma((3,)),
        ],
        compiler_params=pltpu.CompilerParams(collective_id=0, has_side_effects=True),
        name="coupling",
    )(offsets, reflectors, eigvec)
    sets, coef, off, x = (pltpu.with_memory_space_constraint(array, pltpu.VMEM) for array in held)
    steps = 4
    return pl.pallas_call(
        update_kernel,
        out_shape=jax.ShapeDtypeStruct(eigvec.shape, f32),
        in_specs=[vmem, vmem, vmem, vmem],
        out_specs=hbm,
        scratch_shapes=[pltpu.VMEM((steps, rows // steps, cols), f32), dma((steps,))],
        name="update",
    )(off, sets, coef, x)


def solution(mesh):
    in_specs = (P(("grp", "row"), "col"), P(None, ("grp", "row", "col")), P("grp"))
    out_specs = P(("grp", "row"), "col")
    step = functools.partial(body, mesh.shape["col"], mesh.shape["row"])
    return jax.shard_map(step, mesh=mesh, in_specs=in_specs, out_specs=out_specs, check_vma=False)
```

```python
import functools

import jax
import jax.numpy as jnp
from jax import lax
from jax.experimental import pallas as pl
from jax.experimental.pallas import tpu as pltpu
from jax.sharding import PartitionSpec as P

B = 256
MESH = pl.DeviceIdType.MESH
HIGHEST = lax.Precision.HIGHEST


def masked_sets(tile, off, first_row, group):
    row = first_row + lax.broadcasted_iota(jnp.int32, tile.shape, 1) - group * B
    tile = jnp.where(row == off, 1.0, tile)
    before = row < off
    return jnp.concatenate([jnp.where(before, tile, 0.0), jnp.where(before, 0.0, tile)], 0)


def offset_column(off_ref, sweeps):
    which = lax.broadcasted_iota(jnp.int32, (sweeps, 1), 0)
    off = jnp.zeros((sweeps, 1), jnp.int32)
    for s in range(sweeps):
        off = jnp.where(which == s, off_ref[s], off)
    return off


def halves(x):
    high = x.astype(jnp.bfloat16)
    return high, (x - high.astype(jnp.float32)).astype(jnp.bfloat16)


def product(v, x):
    count = v.shape[0]
    v_high, v_low = halves(v)
    x_high, x_low = halves(x)
    both = jnp.dot(jnp.concatenate([v_high, v_low], 0), x_high, preferred_element_type=jnp.float32)
    return both[:count] + both[count:] + jnp.dot(v_high, x_low, preferred_element_type=jnp.float32)


def coupling_kernel(
    n_col, n_row, off_hbm, refl_hbm, eig_hbm, sets_ref, coef_ref, off_ref, x_ref,
    sets, own, chain, side, tails, off_smem, sent, passed, recv, row_send, row_recv, side_send, side_recv, tail_send, tail_recv, loaded,
):
    sweeps, chunk = refl_hbm.shape
    rows, cols = eig_hbm.shape
    blocks, parts = rows // B, cols // 128
    per_block = B // chunk
    col = lax.axis_index("col")
    row = lax.axis_index("row")
    has_above, has_below = row > 0, row < n_row - 1
    end, head = n_col - 1, n_col - per_block
    apart = (row == 0) & (lax.axis_index("grp") == 0)

    loads = [
        pltpu.make_async_copy(refl_hbm, sets.at[col], loaded.at[0]),
        pltpu.make_async_copy(off_hbm, off_smem, loaded.at[1]),
        pltpu.make_async_copy(eig_hbm, x_ref, loaded.at[2]),
    ]
    for load in loads:
        load.start()

    barrier = pltpu.get_barrier_semaphore()

    def greet(axis, peer):
        pl.semaphore_signal(barrier, inc=1, device_id={axis: peer}, device_id_type=MESH)

    @pl.when(has_above)
    def _():
        greet("row", row - 1)

    @pl.when(has_below)
    def _():
        greet("row", row + 1)

    @pl.when((col == 0) & jnp.logical_not(apart))
    def _():
        greet("col", 1)

    @pl.when((col == 1) & apart)
    def _():
        greet("col", 2)

    peers = jnp.where(has_above, 1, 0) + jnp.where(has_below, 1, 0) + jnp.where(col == 0, 0, 1) + jnp.where(col == end, 1, 0)
    pl.semaphore_wait(barrier, peers)

    @pl.when((col == 0) & apart)
    def _():
        greet("col", 1)

    @pl.when(col == 0)
    def _():
        greet("col", end)

    @pl.when(((col >= 2) | ((col == 1) & jnp.logical_not(apart))) & (col < end))
    def _():
        greet("col", col + 1)

    def remote(source, target, send_sem, recv_sem, **device):
        return pltpu.make_async_remote_copy(
            src_ref=source, dst_ref=target, send_sem=send_sem, recv_sem=recv_sem, device_id=device, device_id_type=MESH
        )

    def block_to(peer):
        return remote(sets.at[col], sets.at[col], sent.at[peer], recv.at[col], col=peer)

    def passed_on(index):
        return remote(sets.at[index], sets.at[index], passed.at[index], recv.at[index], col=0)

    def arrived(index):
        remote(sets.at[index], sets.at[index], sent.at[index], recv.at[index], col=index).wait_recv()

    above, below = jnp.maximum(row - 1, 0), jnp.minimum(row + 1, n_row - 1)

    def aside(which, peer_col, upward, extra=0):
        slot, peer = (1, above) if upward else (0, below)
        target, index = side.at[slot, which], slot * per_block + which
        return remote(sets.at[head + which], target, side_send.at[index + extra], side_recv.at[index], row=peer, col=peer_col)

    def asides(which, peer_col, act, extra=0):
        @pl.when(has_below)
        def _():
            act(aside(which, peer_col, False, extra))

        @pl.when(has_above)
        def _():
            act(aside(which, peer_col, True, extra))

    def start(copy):
        copy.start()

    def sent_off(copy):
        copy.wait_send()

    loads[0].wait()

    relay, served = (col == 1) & apart, (col == 0) & apart

    def forwards(which):
        return col > 0 if which == per_block - 1 else jnp.logical_not(served)

    to_first = (col == 1) | (col == end) | ((col > 0) & jnp.logical_not(apart))

    @pl.when(to_first)
    def _():
        block_to(0).start()

    @pl.when(relay)
    def _():
        for peer in range(2, head):
            arrived(peer)
            passed_on(peer).start()
        for peer in range(2, head):
            block_to(peer).start()
        for which in range(per_block - 1):
            arrived(head + which)
            passed_on(head + which).start()
            asides(which, 0, start, 2 * per_block)
            block_to(head + which).start()

    @pl.when(col == end)
    def _():
        asides(per_block - 1, 0, start, 2 * per_block)

    for peer in range(1, end):

        @pl.when(peer < col)
        def _():
            block_to(peer).start()

    for which in range(per_block):

        @pl.when(col == head + which)
        def _():
            asides(which, col, start)

    loads[1].wait()
    off = offset_column(off_smem, sweeps)
    off_ref[...] = jnp.broadcast_to(off, off_ref.shape)
    own[...] = jnp.zeros_like(own)
    chain_rows = chain.shape[1]

    def project(tile, first, b, x):
        v = masked_sets(tile, off, first, b)
        p = product(v, x)
        padded = [jnp.zeros((sweeps, v.shape[1]), jnp.float32), v, jnp.zeros((128 - 3 * sweeps, v.shape[1]), jnp.float32)]
        g = lax.dot_general(
            v, jnp.concatenate(padded, 0), (((1,), (1,)), ((), ())), precision=HIGHEST, preferred_element_type=jnp.float32
        )
        g = jnp.concatenate([g[:sweeps], pltpu.roll(g[sweeps:], 128 - sweeps, 1)], 0)
        return [p[:, h * 128 : (h + 1) * 128] for h in range(parts)] + [g]

    def project_own(first_chunk, count):
        b = first_chunk // per_block
        tile = jnp.concatenate([sets[first_chunk + i] for i in range(count)], 1)
        terms = project(tile, first_chunk * chunk, b, x_ref[first_chunk * chunk : (first_chunk + count) * chunk])
        for h, term in enumerate(terms):
            own[h, b * sweeps : (b + 2) * sweeps] += term

    groups = blocks + 1
    seam, other = (groups - 2) * sweeps, (2 * groups - 3) * sweeps
    below_end = other + (groups - 1) * sweeps

    def down():
        return remote(own.at[:, sweeps:], chain.at[:, : seam + sweeps], row_send.at[0], row_recv.at[0], row=below)

    def up():
        source = own.at[:, : (groups - 1) * sweeps]
        return remote(source, chain.at[:, other:below_end], row_send.at[1], row_recv.at[1], row=above)

    def tail_down():
        return remote(x_ref.at[rows - B :], tails.at[0], tail_send.at[0], tail_recv.at[0], row=below)

    def tail_up():
        return remote(x_ref.at[rows - B :], tails.at[1], tail_send.at[1], tail_recv.at[1], row=above)

    def to_rows():
        @pl.when(has_below)
        def _():
            down().start()

        @pl.when(has_above)
        def _():
            up().start()

    loads[2].wait()

    @pl.when(has_below)
    def _():
        tail_down().start()

    @pl.when(has_above)
    def _():
        tail_up().start()

    def answered(peer):
        @pl.when((peer > col) & (jnp.logical_not(relay) if 2 <= peer < end else (col >= 0)))
        def _():
            arrived(peer)

        def answer():
            block_to(peer).start()

        now = (peer > col) & (jnp.logical_not(relay) if 2 <= peer < end else (col >= 0))
        if 2 <= peer < head:
            now &= jnp.logical_not(served)
        pl.when(now)(answer)

    def early_sent():
        for peer in range(head):

            @pl.when((peer != col) & (to_first if peer == 0 else (col >= 0)))
            def _():
                block_to(peer).wait_send()

        @pl.when(relay)
        def _():
            for peer in range(2, end):
                passed_on(peer).wait_send()
            for which in range(per_block - 1):
                asides(which, 0, sent_off, 2 * per_block)

        @pl.when(has_below)
        def _():
            tail_down().wait_send()

        @pl.when(has_above)
        def _():
            tail_up().wait_send()

    for peer in range(head):
        answered(peer)
        if peer % per_block == per_block - 1:

            @pl.when(peer - per_block + 1 >= col)
            def _():
                project_own(peer - per_block + 1, per_block)

    for first in range(0, head, per_block):
        for peer in range(first, first + per_block):

            @pl.when(peer < col)
            def _():
                arrived(peer)

        @pl.when(first < col)
        def _():
            project_own(first, per_block)

    to_rows()

    @pl.when(served)
    def _():
        for peer in range(2, head):
            block_to(peer).start()

    for which in range(per_block):
        if which == per_block - 1:
            early_sent()
        peer = head + which
        answered(peer)

        @pl.when(peer < col)
        def _():
            arrived(peer)

        @pl.when((peer != col) & forwards(which))
        def _():
            asides(which, col, start)

    chain[:, seam + sweeps : other] = own[:, sweeps : (groups - 1) * sweeps]
    chain[:, below_end:] = jnp.zeros((parts + 1, chain_rows - below_end, 128), jnp.float32)

    @pl.when(jnp.logical_not(has_above))
    def _():
        chain[:, : seam + sweeps] = jnp.zeros((parts + 1, seam + sweeps, 128), jnp.float32)
        side[0] = jnp.zeros(side.shape[1:], jnp.float32)
        tails[0] = jnp.zeros_like(tails[0])

    @pl.when(jnp.logical_not(has_below))
    def _():
        chain[:, other:below_end] = jnp.zeros((parts + 1, below_end - other, 128), jnp.float32)
        side[1] = jnp.zeros(side.shape[1:], jnp.float32)
        tails[1] = jnp.zeros_like(tails[1])

    last = rows - B
    mine = project(jnp.concatenate([sets[head + i] for i in range(per_block)], 1), last, blocks - 1, x_ref[last:])

    @pl.when(has_above)
    def _():
        tail_down().wait_recv()
        for which in range(per_block):
            aside(which, col, False).wait_recv()

    @pl.when(has_below)
    def _():
        tail_up().wait_recv()
        for which in range(per_block):
            aside(which, col, True).wait_recv()

    theirs = [
        project(jnp.concatenate([side[slot, i] for i in range(per_block)], 1), last, blocks - 1, tails[slot]) for slot in range(2)
    ]

    @pl.when(has_above)
    def _():
        down().wait_recv()

    @pl.when(has_below)
    def _():
        up().wait_recv()

    for h in range(parts + 1):
        chain[h, seam : seam + sweeps] += own[h, :sweeps] + theirs[0][h][sweeps:]
        chain[h, seam - sweeps : seam] += theirs[0][h][:sweeps]
        chain[h, other - sweeps : other] += mine[h][:sweeps]
        chain[h, other : other + sweeps] += own[h, (groups - 1) * sweeps :] + mine[h][sweeps:]
        chain[h, below_end - sweeps : below_end] += theirs[1][h][:sweeps]

    own_at = groups - 2
    total = chain_rows // sweeps
    place = lax.broadcasted_iota(jnp.int32, (total, 1), 0)
    first = jnp.where(has_above, 0, own_at + 1)
    stop = jnp.where(has_below, own_at + 2 * groups - 2, own_at + groups - 1)
    valid = (place >= first) & (place < stop)
    most = coef_ref.shape[1] // sweeps
    solved = []
    for s in range(sweeps):
        gram = chain[parts, pl.ds(s, total, stride=sweeps), :]
        acc = jnp.concatenate([chain[h, pl.ds(s, total, stride=sweeps), :] for h in range(parts)], 1)
        for p in range(s):
            before, here, after = solved[p]
            acc -= gram[:, sweeps + p : sweeps + p + 1] * here
            acc -= gram[:, p : p + 1] * before
            acc -= gram[:, 2 * sweeps + p : 2 * sweeps + p + 1] * after
        square = gram[:, sweeps + s : sweeps + s + 1]
        tau = jnp.where(valid, 2.0 / jnp.where(valid, square, 1.0), 0.0)
        here = tau * acc
        solved.append((pltpu.roll(here, 1, 0), here, pltpu.roll(here, total - 1, 0)))
        kept = pltpu.roll(here, total - own_at, 0)[:most]
        for h in range(parts):
            coef_ref[h, pl.ds(s, most, stride=sweeps), :] = kept[:, h * 128 : (h + 1) * 128]
    for i in range(n_col):
        sets_ref[i] = sets[i]

    for peer in range(head, n_col):

        @pl.when(peer != col)
        def _():
            block_to(peer).wait_send()

    for which in range(per_block):

        @pl.when(forwards(which))
        def _():
            asides(which, col, sent_off)

    @pl.when(col == end)
    def _():
        asides(per_block - 1, 0, sent_off, 2 * per_block)

    @pl.when(has_below)
    def _():
        down().wait_send()

    @pl.when(has_above)
    def _():
        up().wait_send()


def update_kernel(off_ref, sets_ref, coef_ref, x_ref, out_hbm, out, out_sem):
    count, sweeps, chunk = sets_ref.shape
    per_block = B // chunk
    off = off_ref[:, :1]
    steps = out.shape[0]
    blocks = count // per_block // steps

    def write(step):
        return pltpu.make_async_copy(out.at[step], out_hbm.at[pl.ds(step * blocks * B, blocks * B)], out_sem.at[step])

    for step in range(steps):
        for i in range(blocks):
            b = step * blocks + i
            tile = jnp.concatenate([sets_ref[b * per_block + j] for j in range(per_block)], 1)
            v_high, v_low = halves(masked_sets(tile, off, b * B, b))
            z = [coef_ref[h, b * sweeps : (b + 2) * sweeps, :] for h in range(coef_ref.shape[0])]
            z_high, z_low = halves(jnp.concatenate(z, 1))
            out[step, i * B : (i + 1) * B] = x_ref[b * B : (b + 1) * B] - lax.dot_general(
                jnp.concatenate([v_high, v_low, v_high], 0),
                jnp.concatenate([z_high, z_high, z_low], 0),
                (((0,), (0,)), ((), ())),
                preferred_element_type=jnp.float32,
            )
        write(step).start()
    for step in range(steps):
        write(step).wait()


def body(n_col, n_row, eigvec, reflectors, offsets):
    rows, cols = eigvec.shape
    sweeps, chunk = reflectors.shape
    groups = rows // B + 1
    total, most = (-(-count // 8) * 8 for count in (3 * groups - 3, groups))
    vmem, hbm = pl.BlockSpec(memory_space=pltpu.VMEM), pl.BlockSpec(memory_space=pl.ANY)
    parts, per_block = cols // 128, B // chunk
    dma, f32 = pltpu.SemaphoreType.DMA, jnp.float32
    held = pl.pallas_call(
        functools.partial(coupling_kernel, n_col, n_row),
        out_shape=(
            pltpu.VMEM((n_col, sweeps, chunk), f32),
            pltpu.VMEM((parts, most * sweeps, 128), f32),
            pltpu.VMEM((sweeps, 128), jnp.int32),
            pltpu.VMEM(eigvec.shape, f32),
        ),
        in_specs=[hbm, hbm, hbm],
        out_specs=(vmem, vmem, vmem, vmem),
        scratch_shapes=[
            pltpu.VMEM((n_col, sweeps, chunk), f32),
            pltpu.VMEM((parts + 1, groups * sweeps, 128), f32),
            pltpu.VMEM((parts + 1, total * sweeps, 128), f32),
            pltpu.VMEM((2, per_block, sweeps, chunk), f32),
            pltpu.VMEM((2, B, cols), f32),
            pltpu.SMEM(offsets.shape, jnp.int32),
            dma((n_col,)),
            dma((n_col,)),
            dma((n_col,)),
            dma((2,)),
            dma((2,)),
            dma((4 * per_block,)),
            dma((2 * per_block,)),
            dma((2,)),
            dma((2,)),
            dma((3,)),
        ],
        compiler_params=pltpu.CompilerParams(collective_id=0, has_side_effects=True),
        name="coupling",
    )(offsets, reflectors, eigvec)
    sets, coef, off, x = (pltpu.with_memory_space_constraint(array, pltpu.VMEM) for array in held)
    steps = 4
    return pl.pallas_call(
        update_kernel,
        out_shape=jax.ShapeDtypeStruct(eigvec.shape, f32),
        in_specs=[vmem, vmem, vmem, vmem],
        out_specs=hbm,
        scratch_shapes=[pltpu.VMEM((steps, rows // steps, cols), f32), dma((steps,))],
        name="update",
    )(off, sets, coef, x)


def solution(mesh):
    in_specs = (P(("grp", "row"), "col"), P(None, ("grp", "row", "col")), P("grp"))
    out_specs = P(("grp", "row"), "col")
    step = functools.partial(body, mesh.shape["col"], mesh.shape["row"])
    return jax.shard_map(step, mesh=mesh, in_specs=in_specs, out_specs=out_specs, check_vma=False)
```
